512 devices in a mesh: section: 8 (over x, core), dp: 32 (over z, y_lo), mp: 2 (over y_hi).
Axes of the slice: x: 4, y: 4 (y_hi: 2, y_lo: 2; y = y_hi * 2 + y_lo), z: 16, core: 2. Of those that a mesh axis runs over, the one named last changes fastest.
Arguments:
- layer_inputs: bfloat16 [8, 128, 4096], P('section', None, 'mp'), may hold values from -6 to 6
- pre_act: bfloat16 [8, 128, 8192], P('section', None, 'dp'), may hold values from -6 to 6
- out_grad: bfloat16 [128, 4096], P(None, 'mp'), may hold values from -4 to 4
- w_in: bfloat16 [32, 8, 32, 4096], P('dp', 'section', None, 'mp'), may hold values from -0.09375 to 0.09375
- w_out: bfloat16 [32, 8, 32, 4096], P('dp', 'section', None, 'mp'), may hold values from -0.0625 to 0.0625
Outputs:
- in_grads: bfloat16 [8, 128, 4096], P('section', None, 'mp')
- grad_in: float32 [32, 8, 32, 4096], P('dp', 'section', None, 'mp')
- grad_out: float32 [32, 8, 32, 4096], P('dp', 'section', None, 'mp')
The draws below stay inside these ranges and needn't reach their ends.
All inputs are finite; a program needn't handle non-finite values.
Results may differ from the reference program's by a relative error of at most 0.035.
Values may be sent and summed in bfloat16 or wider, within the bound.
No kernel may reach another device: no remote copies, remote signals or barrier semaphores. Data moves between devices by JAX's collectives and lax.ppermute only.
A program may use at most 64 MiB of HBM per device.

```python
import jax
import jax.numpy as jnp
from jax import lax

D = 4096
FF = 8192
TOKS = 128
SECTIONS = 8
FB = 32
N_SECTION = 8
N_DP = 32
N_MP = 2


def block_levels(rng, shape, shards, low, largest):
    gain, own = 1.0, jax.random.fold_in(rng, 6)
    for dim, blocks in shards:
        draws = jnp.exp(jax.random.uniform(jax.random.fold_in(own, dim), (blocks,), jnp.float32, low / len(shards), largest / len(shards)))
        gain = gain * jnp.repeat(draws, shape[dim] // blocks).reshape([-1 if axis == dim else 1 for axis in range(len(shape))])
    return gain


def centred(stream_key, extent, scale, bound, split=(), held_as=jnp.bfloat16):
    level = block_levels(stream_key, extent, split, -0.22, 0.18) if split else 1.0
    entries = jax.random.normal(stream_key, extent, jnp.float32) * scale * level
    return jnp.minimum(jnp.maximum(entries, -bound), bound).astype(held_as)


def setup_inputs(seed: int = 0) -> dict:
    streams_of = jax.random.split(jax.random.key(seed), 6)
    layer_inputs = centred(streams_of[0], (SECTIONS, TOKS, D), 1.0, 6.0, ((0, 8), (2, 2)))
    pre_act = centred(streams_of[1], (SECTIONS, TOKS, FF), 1.0, 6.0, ((0, 8), (2, 32)))
    out_grad = centred(streams_of[2], (TOKS, D), 0.3, 4.0, ((1, 2),))
    w_in = centred(streams_of[3], (N_DP, N_SECTION, FB, D), D ** -0.5, 0.09375, ((0, 32), (1, 8), (3, 2)))
    w_out = centred(streams_of[4], (N_DP, N_SECTION, FB, D), FF ** -0.5, 0.0625, ((0, 32), (1, 8), (3, 2)))
    return dict(layer_inputs=layer_inputs, pre_act=pre_act, out_grad=out_grad, w_in=w_in, w_out=w_out)


def gelu_slope(value):
    cdf = 0.5 * (1.0 + lax.erf(value * 0.7071067811865476))
    dens = jnp.exp(-0.5 * value * value) * 0.3989422804014327
    return cdf + value * dens


def rounded(value):
    return lax.optimization_barrier(value.astype(jnp.bfloat16)).astype(jnp.float32)


def reference(layer_inputs, pre_act, out_grad, w_in, w_out):
    in_rows = w_in.reshape(FF, D)
    out_rows = w_out.reshape(FF, D)
    feat = D // N_MP
    units = FF // N_DP
    upper = out_grad
    grad_in = jnp.zeros((FF, D), jnp.float32)
    grad_out = jnp.zeros((FF, D), jnp.float32)
    results = []
    for spot in reversed(range(SECTIONS)):
        back = jnp.zeros((TOKS, FF), jnp.float32)
        for block in range(N_MP):
            piece = jnp.dot(upper[:, block * feat:(block + 1) * feat], out_rows[:, block * feat:(block + 1) * feat].T, preferred_element_type=jnp.float32)
            back = back + rounded(piece)
        saved = pre_act[spot].astype(jnp.float32)
        gee = (back * gelu_slope(saved)).astype(jnp.bfloat16)
        total = upper.astype(jnp.float32)
        for block in range(N_DP):
            piece = jnp.dot(gee[:, block * units:(block + 1) * units], in_rows[block * units:(block + 1) * units, :], preferred_element_type=jnp.float32)
            total = total + rounded(piece)
        result = total.astype(jnp.bfloat16)
        hidden = jax.nn.gelu(saved, approximate=False).astype(jnp.bfloat16)
        grad_in = grad_in + rounded(jnp.dot(gee.T, layer_inputs[spot], preferred_element_type=jnp.float32))
        grad_out = grad_out + rounded(jnp.dot(hidden.T, upper, preferred_element_type=jnp.float32))
        results.append(result)
        upper = result
    in_grads = jnp.stack(results[::-1], axis=0)
    return (in_grads, grad_in.reshape(N_DP, N_SECTION, FB, D), grad_out.reshape(N_DP, N_SECTION, FB, D))
```

```python
import jax
import jax.numpy as jnp
from jax import lax
from jax.sharding import Mesh
from jax.sharding import PartitionSpec as P

F32 = jnp.float32
BF16 = jnp.bfloat16
SEC = ("x", "core")
DP = ("z", "yl")
TOK = ("z", "core")
ROWS = ("x", "yl")


def size(axes):
    n = 1
    for a in axes:
        n *= lax.axis_size(a)
    return n


def shared(value, axes):
    n = size(axes)
    return lax.all_to_all(
        jnp.broadcast_to(value[None], (n,) + value.shape), axes, 0, 0, tiled=True
    )


def gelu_slope(value):
    cdf = 0.5 * (1.0 + lax.erf(value * 0.7071067811865476))
    dens = jnp.exp(-0.5 * value * value) * 0.3989422804014327
    return cdf + value * dens


def dot(left, right, dims):
    return lax.dot_general(left, right, (dims, ((), ())), preferred_element_type=F32)


def body(layer_inputs, pre_act, out_grad, w_in, w_out):
    nx, nc, nz, nyl = (lax.axis_size(a) for a in ("x", "core", "z", "yl"))
    sections, groups = nx * nc, nz * nc
    tok_rows, width = out_grad.shape
    per = w_in.shape[2]
    each = tok_rows // groups
    units = groups * per
    own_in = w_in.reshape(per, width)
    own_out = w_out.reshape(per, width)
    saved = pre_act[0]
    spot = lax.axis_index(SEC)
    mine = lax.axis_index(TOK)

    both = lax.all_gather(jnp.concatenate([own_out, own_in], 0), TOK, axis=0)
    rows_out = both[:, :per].reshape(units, width)
    rows_in = both[:, per:].reshape(units, width)
    inputs = lax.all_gather(layer_inputs[0], SEC, axis=0)

    own_pre = lax.all_to_all(
        saved.reshape(tok_rows, sections, per).transpose(1, 0, 2), SEC, 0, 0, tiled=True
    ).astype(F32)
    part = dot(out_grad, own_out, ((1,), (1,))).astype(BF16)
    back = lax.all_gather(part, "mp").astype(F32).sum(0)
    gee_last = (back * gelu_slope(own_pre[sections - 1])).astype(BF16)
    gee = lax.all_to_all(gee_last.reshape(groups, each, per), TOK, 0, 0, tiled=True)
    gee = gee.transpose(1, 0, 2).reshape(each, units)
    sent = saved.reshape(nz, nc, each, nx, nc, per).transpose(3, 1, 0, 2, 4, 5)
    sent = sent.reshape(nx * nc * nz, each * nc * per // 128, 128)
    got = lax.all_to_all(sent, ("x", "core", "z"), 0, 0, tiled=True)
    got = got.reshape(sections, nz, each, nc, per).transpose(0, 2, 1, 3, 4)
    slopes = gelu_slope(got.reshape(sections, each, units).astype(F32))

    upper = lax.dynamic_slice_in_dim(out_grad, mine * each, each, 0)
    gees, results = [], []
    for s in reversed(range(sections)):
        if s < sections - 1:
            part = dot(upper, rows_out, ((1,), (1,))).astype(BF16)
            back = lax.all_gather(part, "mp").astype(F32).sum(0)
            gee = (back * slopes[s]).astype(BF16)
            gees.append(gee)
        branch = dot(gee, rows_in, ((1,), (0,))).astype(BF16)
        total = shared(branch, ROWS).astype(F32).sum(0)
        upper = (upper.astype(F32) + total).astype(BF16)
        results.append(upper)
    early = jnp.concatenate(results[: sections - 2], 0)
    early = lax.all_gather(early, TOK, axis=0).reshape(groups, sections - 2, each, width)
    late = []
    for r in results[sections - 2 :]:
        r = shared(r, ("z",))
        r = lax.all_gather(r, "core", axis=1)
        late.append(r.reshape(groups, 1, each, width))
    grads = jnp.concatenate([early] + late, 1)

    gs = jnp.stack(gees, 0).reshape(sections - 1, each, groups, per).transpose(2, 0, 1, 3)
    gs = lax.all_to_all(gs.reshape(groups, -1, 128), TOK, 0, 0, tiled=True)
    gs = gs.reshape(groups, sections - 1, each, per).transpose(1, 0, 2, 3)
    gs = jnp.concatenate([gee_last[None], gs.reshape(sections - 1, tok_rows, per)], 0)[::-1]
    grad_in = dot(
        gs.reshape(sections * tok_rows, per),
        inputs.reshape(sections * tok_rows, width),
        ((0,), (0,)),
    )
    hidden = jax.nn.gelu(own_pre, approximate=False).astype(BF16)
    low = hidden[: sections - 1][::-1].reshape(sections - 1, groups, each, per)
    low = low.transpose(1, 0, 2, 3).reshape(-1, per)
    grad_out = dot(hidden[sections - 1], out_grad, ((0,), (0,))) + dot(
        low, grads[:, : sections - 1].reshape(-1, width), ((0,), (0,))
    )
    in_grads = lax.dynamic_index_in_dim(grads, sections - 1 - spot, 1, False)
    return (
        in_grads.reshape(1, tok_rows, width),
        grad_in.reshape(w_in.shape),
        grad_out.reshape(w_out.shape),
    )


def solution(mesh):
    split = Mesh(
        mesh.devices.reshape(
            mesh.shape["section"] // 2, 2, mesh.shape["dp"] // 2, 2, mesh.shape["mp"]
        ),
        ("x", "core", "z", "yl", "mp"),
    )
    placed = (
        P(SEC, None, "mp"),
        P(SEC, None, DP),
        P(None, "mp"),
        P(DP, SEC, None, "mp"),
        P(DP, SEC, None, "mp"),
    )
    return jax.shard_map(
        body,
        mesh=split,
        in_specs=placed,
        out_specs=(P(SEC, None, "mp"), P(DP, SEC, None, "mp"), P(DP, SEC, None, "mp")),
        check_vma=False,
    )
```

```python
import jax
import jax.numpy as jnp
from jax import lax
from jax.sharding import Mesh
from jax.sharding import PartitionSpec as P

F32 = jnp.float32
BF16 = jnp.bfloat16
LANES = 128
SEC = ("x", "core")
DP = ("z", "yl")
TOK = ("z", "core")
ROWS = ("x", "yl")


def size(axes):
    n = 1
    for a in axes:
        n *= lax.axis_size(a)
    return n


def exchange(value, axes):
    return lax.all_to_all(value, axes, 0, 0, tiled=True)


def shared(value, axes):
    n = size(axes)
    return exchange(jnp.broadcast_to(value[None], (n,) + value.shape), axes)


def fence(*values):
    return lax.optimization_barrier(values if len(values) > 1 else values[0])


def gelu_slope(value):
    cdf = 0.5 * (1.0 + lax.erf(value * 0.7071067811865476))
    dens = jnp.exp(-0.5 * value * value) * 0.3989422804014327
    return cdf + value * dens


def dot(left, right, dims):
    return lax.dot_general(left, right, (dims, ((), ())), preferred_element_type=F32)


def body(layer_inputs, pre_act, out_grad, w_in, w_out):
    nc, nz = lax.axis_size("core"), lax.axis_size("z")
    sections, groups = size(SEC), nz * nc
    tok_rows, width = out_grad.shape
    per = w_in.shape[2]
    each = tok_rows // groups
    units = groups * per
    last = sections - 1
    own_in = w_in.reshape(per, width)
    own_out = w_out.reshape(per, width)
    spot = lax.axis_index(SEC)
    mine = lax.axis_index(TOK)

    both = lax.all_gather(jnp.concatenate([own_out, own_in], 0), TOK, axis=0)
    inputs = lax.all_gather(layer_inputs[0], SEC, axis=0)

    own_pre = exchange(
        pre_act[0].reshape(tok_rows, sections, per).transpose(1, 0, 2), SEC
    )
    part = dot(out_grad, own_out, ((1,), (1,))).astype(BF16)
    back = lax.all_gather(part, "mp").astype(F32).sum(0)
    gee_last = (back * gelu_slope(own_pre[last].astype(F32))).astype(BF16)
    sent = jnp.concatenate([own_pre[:last], gee_last[None]], 0)
    sent = sent.reshape(sections, groups, each * per // LANES, LANES)
    got = exchange(sent.transpose(1, 0, 2, 3).reshape(groups, -1, LANES), TOK)
    got = got.reshape(groups, sections, each, per).transpose(1, 2, 0, 3)
    got = got.reshape(sections, each, units)
    gee = got[last]
    slopes = gelu_slope(got[:last].astype(F32))
    upper = lax.dynamic_slice_in_dim(out_grad, mine * each, each, 0)
    hidden = jax.nn.gelu(own_pre.astype(F32), approximate=False).astype(BF16)
    hidden_rows = hidden[1:last].reshape(last - 1, groups, each, per)[::-1]
    hidden_rows = hidden_rows.transpose(1, 0, 2, 3).reshape(-1, per)

    slopes = [slopes[s] for s in range(last)]
    both, gee, upper, hidden_rows, *slopes = fence(both, gee, upper, hidden_rows, *slopes)
    rows_in, rows_out = fence(
        both[:, per:].reshape(units, width), both[:, :per].reshape(units, width)
    )

    gees, results = [], []
    for s in reversed(range(sections)):
        if s < last:
            part = dot(upper, rows_out, ((1,), (1,))).astype(BF16)
            back = lax.all_gather(part, "mp").astype(F32).sum(0)
            gee = fence((back * slopes[s]).astype(BF16))
            gees.append(gee)
        branch = dot(gee, rows_in, ((1,), (0,))).astype(BF16)
        total = shared(branch, ROWS).astype(F32).sum(0)
        upper = fence((upper.astype(F32) + total).astype(BF16))
        results.append(upper)
        if s == 2:
            early = lax.all_gather(jnp.concatenate(results, 0), TOK, axis=0)
            early = early.reshape(groups * (last - 1) * each, width)

    *gees, second, first = fence(*gees, results[-2], results[-1])
    gs = jnp.stack(gees, 0).reshape(last, each, nz, nc * per)
    gs = gs.transpose(2, 0, 1, 3).reshape(nz, -1, LANES)
    n_gs = gs.shape[1]
    n_res = each * width // LANES
    late = jnp.concatenate([second.reshape(-1, LANES), first.reshape(-1, LANES)], 0)
    late = jnp.concatenate([jnp.broadcast_to(late[None], (nz,) + late.shape), gs], 1)
    late = jnp.pad(late, ((0, 0), (0, -late.shape[1] % 8), (0, 0)))
    late = exchange(late, "z")
    first = lax.all_gather(late[:, n_res : 2 * n_res], "core", axis=1).reshape(tok_rows, width)
    second = lax.all_gather(late[:, :n_res], "core", axis=1).reshape(tok_rows, width)
    gs = lax.all_gather(late[:, 2 * n_res : 2 * n_res + n_gs], "core", axis=1)
    gs = gs.reshape(groups, last, each, nc, per)
    gs = lax.dynamic_index_in_dim(gs, lax.axis_index("core"), 3, False)
    gs = gs.transpose(1, 0, 2, 3).reshape(last, tok_rows, per)[::-1]
    gs = jnp.concatenate([gs, gee_last[None]], 0)

    grad_in = dot(
        gs.reshape(sections * tok_rows, per),
        inputs.reshape(sections * tok_rows, width),
        ((0,), (0,)),
    )
    row = lax.broadcasted_iota(jnp.int32, (tok_rows, early.shape[0]), 0)
    col = lax.broadcasted_iota(jnp.int32, (tok_rows, early.shape[0]), 1)
    at = row // each * ((last - 1) * each) + (last - spot) * each + row % each
    pick = jnp.where((col == at) & (spot > 1), 1.0, 0.0).astype(BF16)
    left = jnp.concatenate([pick, hidden_rows.T], 0)
    found = dot(left, early, ((1,), (0,)))
    grad_out = (
        dot(hidden[last], out_grad, ((0,), (0,)))
        + dot(hidden[0], second, ((0,), (0,)))
        + found[tok_rows:]
    )
    in_grads = jnp.where(
        spot == 0, first, jnp.where(spot == 1, second, found[:tok_rows].astype(BF16))
    )
    return (
        in_grads.reshape(1, tok_rows, width),
        grad_in.reshape(w_in.shape),
        grad_out.reshape(w_out.shape),
    )


def solution(mesh):
    split = Mesh(
        mesh.devices.reshape(
            mesh.shape["section"] // 2, 2, mesh.shape["dp"] // 2, 2, mesh.shape["mp"]
        ),
        ("x", "core", "z", "yl", "mp"),
    )
    placed = (
        P(SEC, None, "mp"),
        P(SEC, None, DP),
        P(None, "mp"),
        P(DP, SEC, None, "mp"),
        P(DP, SEC, None, "mp"),
    )
    return jax.shard_map(
        body,
        mesh=split,
        in_specs=placed,
        out_specs=(P(SEC, None, "mp"), P(DP, SEC, None, "mp"), P(DP, SEC, None, "mp")),
        check_vma=False,
    )
```

```python
import jax
import jax.numpy as jnp
from jax import lax
from jax.experimental import pallas as pl
from jax.experimental.pallas import tpu as pltpu
from jax.sharding import Mesh
from jax.sharding import PartitionSpec as P

F32 = jnp.float32
BF16 = jnp.bfloat16
LANES = 128
SEC = ("x", "core")
DP = ("z", "yl")
TOK = ("core", "z")
HID = ("z", "core")
ROWS = ("x", "yl")


def size(axes):
    n = 1
    for a in axes:
        n *= lax.axis_size(a)
    return n


def exchange(value, axes):
    return lax.all_to_all(value, axes, 0, 0, tiled=True)


def shared(value, axes):
    n = size(axes)
    return exchange(jnp.broadcast_to(value[None], (n,) + value.shape), axes)


def fence(*values):
    return lax.optimization_barrier(values if len(values) > 1 else values[0])


def gelu_slope(value):
    cdf = 0.5 * (1.0 + lax.erf(value * 0.7071067811865476))
    dens = jnp.exp(-0.5 * value * value) * 0.3989422804014327
    return cdf + value * dens


def dot(left, right, dims):
    return lax.dot_general(left, right, (dims, ((), ())), preferred_element_type=F32)


def finish_kernel(
    pick_early, pick_late, pick_core, pick_even, pick_odd, gee_last, base, left, right, inputs, early,
    in_grads, grad_in, grad_out,
    x_buf, e_buf, even, odd, sems,
):
    tok_rows, block = in_grads.shape
    per = gee_last.shape[1]
    step, steps = pl.program_id(0), pl.num_programs(0)
    nc, half, rows, piece = left.shape

    def both_cores(value):
        return value.reshape(nc * rows, piece)

    def copies(i):
        cols = pl.ds(pl.multiple_of(i * block, block), block)
        return (
            pltpu.make_async_copy(inputs.at[:, cols], x_buf.at[i], sems.at[0, i]),
            pltpu.make_async_copy(early.at[:, cols], e_buf.at[i], sems.at[1, i]),
        )

    @pl.when(step == 0)
    def _():
        for i in range(x_buf.shape[0]):
            for copy in copies(i):
                copy.start()
        mine = dot(both_cores(right[:, half]), pick_core[...], ((1,), (0,))).astype(BF16)
        even[...] = dot(pick_even[...], mine, ((1,), (0,))).astype(BF16)
        odd[...] = dot(pick_odd[...], mine, ((1,), (0,))).astype(BF16)

    for copy in copies(step):
        copy.wait()
    at = block // piece * (step % (steps // 2))
    late = jnp.concatenate(
        [
            jnp.where(step < steps // 2, both_cores(left[:, at + i]), both_cores(right[:, at + i]))
            for i in range(block // piece)
        ],
        1,
    )
    x = x_buf[step]
    n = x.shape[0] // tok_rows
    total = dot(gee_last[...], x[(n - 1) * tok_rows :], ((0,), (0,)))
    for j in range(n - 1):
        gee = (even, odd)[j % 2][:, j // 2 * per : (j // 2 + 1) * per]
        s = n - 2 - j
        total += dot(gee, x[s * tok_rows : (s + 1) * tok_rows], ((0,), (0,)))
    grad_in[...] = total
    found = dot(pick_early[...], e_buf[step], ((1,), (0,)))
    row = lax.broadcasted_iota(jnp.int32, late.shape, 0)
    second = jnp.where(row % 8 < 4, late.astype(F32), 0.0).astype(BF16)
    picked = dot(pick_late[:tok_rows], late, ((1,), (0,)))
    in_grads[...] = (found[:tok_rows] + picked).astype(BF16)
    grad_out[...] = (
        base[...] + found[tok_rows:] + dot(pick_late[tok_rows:], second, ((1,), (0,)))
    )


def finish(pick_early, pick_late, pick_core, pick_even, pick_odd, gee_last, base, left, right, inputs, early):
    per, width = base.shape
    tok_rows = gee_last.shape[0]
    steps = 4
    block = width // steps
    inputs = pltpu.with_memory_space_constraint(inputs, pltpu.HBM)
    early = pltpu.with_memory_space_constraint(early, pltpu.HBM)
    whole = lambda a: pl.BlockSpec(a.shape, lambda i: (0,) * a.ndim)
    cut = lambda rows: pl.BlockSpec((rows, block), lambda i: (0, i))
    return pl.pallas_call(
        finish_kernel,
        grid=(steps,),
        in_specs=[
            whole(pick_early),
            whole(pick_late),
            whole(pick_core),
            whole(pick_even),
            whole(pick_odd),
            whole(gee_last),
            cut(per),
            whole(left),
            whole(right),
            pl.BlockSpec(memory_space=pltpu.MemorySpace.HBM),
            pl.BlockSpec(memory_space=pltpu.MemorySpace.HBM),
        ],
        out_specs=[cut(tok_rows), cut(per), cut(per)],
        out_shape=[
            jax.ShapeDtypeStruct((tok_rows, width), BF16),
            jax.ShapeDtypeStruct((per, width), F32),
            jax.ShapeDtypeStruct((per, width), F32),
        ],
        scratch_shapes=[
            pltpu.VMEM((steps, inputs.shape[0], block), BF16),
            pltpu.VMEM((steps, early.shape[0], block), BF16),
            pltpu.VMEM((tok_rows, pick_core.shape[1]), BF16),
            pltpu.VMEM((tok_rows, pick_core.shape[1]), BF16),
            pltpu.SemaphoreType.DMA((2, steps)),
        ],
        compiler_params=pltpu.CompilerParams(vmem_limit_bytes=24 << 20),
        name="finish",
    )(pick_early, pick_late, pick_core, pick_even, pick_odd, gee_last, base, left, right, inputs, early)


def body(layer_inputs, pre_act, out_grad, w_in, w_out):
    nc, nz = lax.axis_size("core"), lax.axis_size("z")
    sections, groups = size(SEC), nz * nc
    tok_rows, width = out_grad.shape
    per = w_in.shape[2]
    each = tok_rows // groups
    units = groups * per
    last = sections - 1
    own_in = w_in.reshape(per, width)
    own_out = w_out.reshape(per, width)
    spot = lax.axis_index(SEC)
    mine = lax.axis_index(TOK)

    both = lax.all_gather(jnp.concatenate([own_out, own_in], 0), HID, axis=0)
    inputs = lax.all_gather(layer_inputs[0], SEC, axis=0)

    own_pre = exchange(
        pre_act[0].reshape(tok_rows, sections, per).transpose(1, 0, 2), SEC
    )
    part = dot(out_grad, own_out, ((1,), (1,))).astype(BF16)
    back = lax.all_gather(part, "mp").astype(F32).sum(0)
    gee_last = (back * gelu_slope(own_pre[last].astype(F32))).astype(BF16)
    sent = jnp.concatenate([own_pre[:last], gee_last[None]], 0)
    sent = sent.reshape(sections, groups, each * per // LANES, LANES)
    got = exchange(sent.transpose(1, 0, 2, 3).reshape(groups, -1, LANES), TOK)
    got = got.reshape(nc, nz, sections, each, per).transpose(2, 3, 1, 0, 4)
    got = got.reshape(sections, each, units)
    gee = got[last]
    slopes = gelu_slope(got[:last].astype(F32))
    upper = lax.dynamic_slice_in_dim(out_grad, mine * each, each, 0)
    hidden = jax.nn.gelu(own_pre.astype(F32), approximate=False).astype(BF16)
    hidden_rows = hidden[1:last].reshape(last - 1, groups, each, per)[::-1]
    hidden_rows = hidden_rows.transpose(3, 1, 0, 2).reshape(per, -1)
    token = lax.broadcasted_iota(jnp.int32, (tok_rows, hidden_rows.shape[1]), 0)
    col = lax.broadcasted_iota(jnp.int32, (tok_rows, hidden_rows.shape[1]), 1)
    at = token // each * ((last - 1) * each) + (last - spot) * each + token % each
    pick_early = jnp.where((col == at) & (spot > 1), 1.0, 0.0).astype(BF16)
    pick_early = jnp.concatenate([pick_early, hidden_rows], 0)
    token = lax.broadcasted_iota(jnp.int32, (tok_rows, 2 * tok_rows), 0)
    col = lax.broadcasted_iota(jnp.int32, (tok_rows, 2 * tok_rows), 1)
    at = token // each * (2 * each) + (1 - spot) * each + token % each
    pick_late = jnp.where((col == at) & (spot < 2), 1.0, 0.0).astype(BF16)
    hidden_late = hidden[0].T.reshape(per, groups, 1, each)
    hidden_late = jnp.pad(hidden_late, ((0, 0), (0, 0), (0, 1), (0, 0))).reshape(per, -1)
    pick_late = jnp.concatenate([pick_late, hidden_late], 0)
    at = token // each * (2 * each) + token % each
    pick_even = jnp.where(col == at, 1.0, 0.0).astype(BF16)
    pick_odd = jnp.where(col == at + each, 1.0, 0.0).astype(BF16)
    src = lax.broadcasted_iota(jnp.int32, (sections // 2 * nc * per, sections // 2 * per), 0)
    dst = lax.broadcasted_iota(jnp.int32, src.shape, 1)
    at = (dst // per * nc + lax.axis_index("core")) * per + dst % per
    pick_core = jnp.where(src == at, 1.0, 0.0).astype(BF16)
    base = dot(hidden[last], out_grad, ((0,), (0,)))

    slopes = [slopes[s] for s in range(last)]
    ready = (pick_early, pick_late, pick_core, pick_even, pick_odd, gee_last, base)
    both, gee, upper, *ready = fence(both, gee, upper, *ready, *slopes)
    ready, slopes = ready[:-last], ready[-last:]
    rows_in, rows_out = fence(
        both[:, per:].reshape(units, width), both[:, :per].reshape(units, width)
    )

    gees, results = [], []
    for s in reversed(range(sections)):
        if s < last:
            part = dot(upper, rows_out, ((1,), (1,))).astype(BF16)
            back = lax.all_gather(part, "mp").astype(F32).sum(0)
            gee = fence((back * slopes[s]).astype(BF16))
            gees.append(gee)
        branch = dot(gee, rows_in, ((1,), (0,))).astype(BF16)
        if s > 0:
            total = shared(branch, ROWS).astype(F32).sum(0)
            upper = fence((upper.astype(F32) + total).astype(BF16))
            results.append(upper)
        if s == 2:
            early = lax.all_gather(jnp.concatenate(results, 0), TOK, axis=0)
            early = early.reshape(groups * (last - 1) * each, width)

    cuts = size(ROWS)
    piece = width // cuts
    total = exchange(branch.reshape(each, cuts, piece).transpose(1, 0, 2), ROWS)
    second = lax.dynamic_slice_in_dim(upper, lax.axis_index(ROWS) * piece, piece, 1)
    first = (second.astype(F32) + total.astype(F32).sum(0)).astype(BF16)
    *gees, second, first = fence(*gees, second, first)
    gs = [g.reshape(each, nz, nc * per).transpose(1, 0, 2) for g in gees]
    gs.append(gs[-1])
    gs = jnp.concatenate(
        [jnp.concatenate(gs[0::2], 2), jnp.concatenate(gs[1::2], 2)], 1
    )
    late = jnp.concatenate([second, first], 0)
    late = jnp.concatenate([jnp.broadcast_to(late[None], (nz,) + late.shape), gs], 2)
    late = exchange(late, "z")
    gs = late[:, :, piece:]
    late = shared(late[:, :, :piece], ROWS)
    left = lax.all_gather(late[: cuts // 2], "core", axis=0)
    right = lax.all_gather(jnp.concatenate([late[cuts // 2 :], gs[None]], 0), "core", axis=0)
    in_grads, grad_in, grad_out = finish(
        *ready,
        left.reshape(nc, cuts // 2, -1, piece),
        right.reshape(nc, cuts // 2 + 1, -1, piece),
        inputs.reshape(sections * tok_rows, width),
        early,
    )
    return (
        in_grads.reshape(1, tok_rows, width),
        grad_in.reshape(w_in.shape),
        grad_out.reshape(w_out.shape),
    )


def solution(mesh):
    split = Mesh(
        mesh.devices.reshape(
            mesh.shape["section"] // 2, 2, mesh.shape["dp"] // 2, 2, mesh.shape["mp"]
        ),
        ("x", "core", "z", "yl", "mp"),
    )
    placed = (
        P(SEC, None, "mp"),
        P(SEC, None, DP),
        P(None, "mp"),
        P(DP, SEC, None, "mp"),
        P(DP, SEC, None, "mp"),
    )
    return jax.shard_map(
        body,
        mesh=split,
        in_specs=placed,
        out_specs=(P(SEC, None, "mp"), P(DP, SEC, None, "mp"), P(DP, SEC, None, "mp")),
        check_vma=False,
    )
```

```python
import jax
import jax.numpy as jnp
from jax import lax
from jax.experimental import pallas as pl
from jax.experimental.pallas import tpu as pltpu
from jax.sharding import Mesh
from jax.sharding import PartitionSpec as P

F32 = jnp.float32
BF16 = jnp.bfloat16
LANES = 128
SEC = ("x", "core")
DP = ("z", "yl")
TOK = ("core", "z")
HID = ("z", "core")
ROWS = ("x", "yl")
PLANE = ("x", "yl", "core")


def size(axes):
    n = 1
    for a in axes:
        n *= lax.axis_size(a)
    return n


def exchange(value, axes):
    return lax.all_to_all(value, axes, 0, 0, tiled=True)


def shared(value, axes):
    n = size(axes)
    return exchange(jnp.broadcast_to(value[None], (n,) + value.shape), axes)


def fence(*values):
    return lax.optimization_barrier(values if len(values) > 1 else values[0])


def gelu_slope(value):
    cdf = 0.5 * (1.0 + lax.erf(value * 0.7071067811865476))
    dens = jnp.exp(-0.5 * value * value) * 0.3989422804014327
    return cdf + value * dens


def dot(left, right, dims):
    return lax.dot_general(left, right, (dims, ((), ())), preferred_element_type=F32)


def finish_kernel(
    pick_early, pick_late, pick_core, pick_even, pick_odd, gee_last, base, left, right, inputs, early,
    in_grads, grad_in, grad_out,
    x_buf, e_buf, even, odd, sems,
):
    tok_rows, block = in_grads.shape
    per = gee_last.shape[1]
    step, steps = pl.program_id(0), pl.num_programs(0)
    nc, half, rows, piece = left.shape

    def both_cores(value):
        return value.reshape(nc * rows, piece)

    def copies(i):
        cols = pl.ds(pl.multiple_of(i * block, block), block)
        return (
            pltpu.make_async_copy(inputs.at[:, cols], x_buf.at[i], sems.at[0, i]),
            pltpu.make_async_copy(early.at[:, cols], e_buf.at[i], sems.at[1, i]),
        )

    @pl.when(step == 0)
    def _():
        for i in range(x_buf.shape[0]):
            for copy in copies(i):
                copy.start()
        mine = dot(both_cores(right[:, half]), pick_core[...], ((1,), (0,))).astype(BF16)
        even[...] = dot(pick_even[...], mine, ((1,), (0,))).astype(BF16)
        odd[...] = dot(pick_odd[...], mine, ((1,), (0,))).astype(BF16)

    for copy in copies(step):
        copy.wait()
    at = block // piece * (step % (steps // 2))
    late = jnp.concatenate(
        [
            jnp.where(step < steps // 2, both_cores(left[:, at + i]), both_cores(right[:, at + i]))
            for i in range(block // piece)
        ],
        1,
    )
    x = x_buf[step]
    n = x.shape[0] // tok_rows


    def rows_of(s):
        return x[s * tok_rows : (s + 1) * tok_rows]

    total = dot(gee_last[...], rows_of(n - 1), ((0,), (0,)))
    for j in range(n - 1):
        gee = (even, odd)[j % 2][:, j // 2 * per : (j // 2 + 1) * per]
        total += dot(gee, rows_of(n - 2 - j), ((0,), (0,)))
    grad_in[...] = total
    found = dot(pick_early[...], e_buf[step], ((1,), (0,)))
    row = lax.broadcasted_iota(jnp.int32, late.shape, 0)
    second = jnp.where(row % 8 < 4, late.astype(F32), 0.0).astype(BF16)
    picked = dot(pick_late[:tok_rows], late, ((1,), (0,)))
    in_grads[...] = (found[:tok_rows] + picked).astype(BF16)
    grad_out[...] = (
        base[...] + found[tok_rows:] + dot(pick_late[tok_rows:], second, ((1,), (0,)))
    )


def finish(pick_early, pick_late, pick_core, pick_even, pick_odd, gee_last, base, left, right, inputs, early):
    per, width = base.shape
    tok_rows = gee_last.shape[0]
    steps = 4
    block = width // steps
    inputs = pltpu.with_memory_space_constraint(inputs, pltpu.HBM)
    early = pltpu.with_memory_space_constraint(early, pltpu.HBM)
    whole = lambda a: pl.BlockSpec(a.shape, lambda i: (0,) * a.ndim)
    cut = lambda rows: pl.BlockSpec((rows, block), lambda i: (0, i))
    return pl.pallas_call(
        finish_kernel,
        grid=(steps,),
        in_specs=[
            whole(pick_early),
            whole(pick_late),
            whole(pick_core),
            whole(pick_even),
            whole(pick_odd),
            whole(gee_last),
            cut(per),
            whole(left),
            whole(right),
            pl.BlockSpec(memory_space=pltpu.MemorySpace.HBM),
            pl.BlockSpec(memory_space=pltpu.MemorySpace.HBM),
        ],
        out_specs=[cut(tok_rows), cut(per), cut(per)],
        out_shape=[
            jax.ShapeDtypeStruct((tok_rows, width), BF16),
            jax.ShapeDtypeStruct((per, width), F32),
            jax.ShapeDtypeStruct((per, width), F32),
        ],
        scratch_shapes=[
            pltpu.VMEM((steps, inputs.shape[0], block), BF16),
            pltpu.VMEM((steps, early.shape[0], block), BF16),
            pltpu.VMEM((tok_rows, pick_core.shape[1]), BF16),
            pltpu.VMEM((tok_rows, pick_core.shape[1]), BF16),
            pltpu.SemaphoreType.DMA((2, steps)),
        ],
        compiler_params=pltpu.CompilerParams(vmem_limit_bytes=24 << 20),
        name="finish",
    )(pick_early, pick_late, pick_core, pick_even, pick_odd, gee_last, base, left, right, inputs, early)


def body(layer_inputs, pre_act, out_grad, w_in, w_out):
    nc, nz = lax.axis_size("core"), lax.axis_size("z")
    sections, groups = size(SEC), nz * nc
    tok_rows, width = out_grad.shape
    per = w_in.shape[2]
    each = tok_rows // groups
    units = groups * per
    last = sections - 1
    own_in = w_in.reshape(per, width)
    own_out = w_out.reshape(per, width)
    spot = lax.axis_index(SEC)
    mine = lax.axis_index(TOK)

    both = lax.all_gather(jnp.concatenate([own_out, own_in], 0), HID, axis=0)

    inputs = lax.all_gather(layer_inputs[0], SEC, axis=0)

    own_pre = exchange(
        pre_act[0].reshape(tok_rows, sections, per).transpose(1, 0, 2), SEC
    )
    part = dot(out_grad, own_out, ((1,), (1,))).astype(BF16)
    back = lax.all_gather(part, "mp").astype(F32).sum(0)
    gee_last = (back * gelu_slope(own_pre[last].astype(F32))).astype(BF16)
    cuts = size(PLANE)
    branch = dot(gee_last, own_in, ((1,), (0,))).astype(BF16)
    branch = exchange(branch.reshape(tok_rows, cuts, -1).transpose(1, 0, 2), PLANE)
    branch = branch.astype(F32).sum(0).astype(BF16).reshape(groups, 1, each, LANES)
    sent = own_pre[:last].reshape(last, groups, each * per // LANES, LANES)
    sent = jnp.pad(sent.transpose(1, 0, 2, 3).reshape(groups, -1, LANES), ((0, 0), (0, 1), (0, 0)))
    sent = jnp.concatenate([branch, sent.reshape(groups, -1, each, LANES)], 1)
    got = exchange(sent, TOK)
    branch = got[:, 0].reshape(nc, nz, each, LANES).astype(F32).sum(1).astype(BF16)
    branch = shared(branch.transpose(1, 0, 2).reshape(each, nc * LANES), ROWS)
    total = branch.transpose(1, 0, 2).reshape(each, width)
    pre = got[:, 1:].reshape(groups, -1, LANES)[:, :last]
    pre = pre.reshape(nc, nz, last, each, per).transpose(2, 3, 1, 0, 4)
    slopes = gelu_slope(pre.reshape(last, each, units).astype(F32))
    upper = lax.dynamic_slice_in_dim(out_grad, mine * each, each, 0)
    upper = (upper.astype(F32) + total.astype(F32)).astype(BF16)
    hidden = jax.nn.gelu(own_pre.astype(F32), approximate=False).astype(BF16)
    hidden_rows = hidden[1:last].reshape(last - 1, groups, each, per)[::-1]
    hidden_rows = hidden_rows.transpose(3, 1, 0, 2).reshape(per, -1)
    token = lax.broadcasted_iota(jnp.int32, (tok_rows, hidden_rows.shape[1]), 0)
    col = lax.broadcasted_iota(jnp.int32, (tok_rows, hidden_rows.shape[1]), 1)
    at = token // each * ((last - 1) * each) + (last - spot) * each + token % each
    pick_early = jnp.where((col == at) & (spot > 1), 1.0, 0.0).astype(BF16)
    pick_early = jnp.concatenate([pick_early, hidden_rows], 0)
    token = lax.broadcasted_iota(jnp.int32, (tok_rows, 2 * tok_rows), 0)
    col = lax.broadcasted_iota(jnp.int32, (tok_rows, 2 * tok_rows), 1)
    at = token // each * (2 * each) + (1 - spot) * each + token % each
    pick_late = jnp.where((col == at) & (spot < 2), 1.0, 0.0).astype(BF16)
    hidden_late = hidden[0].T.reshape(per, groups, 1, each)
    hidden_late = jnp.pad(hidden_late, ((0, 0), (0, 0), (0, 1), (0, 0))).reshape(per, -1)
    pick_late = jnp.concatenate([pick_late, hidden_late], 0)
    at = token // each * (2 * each) + token % each
    pick_even = jnp.where(col == at, 1.0, 0.0).astype(BF16)
    pick_odd = jnp.where(col == at + each, 1.0, 0.0).astype(BF16)
    src = lax.broadcasted_iota(jnp.int32, (sections // 2 * nc * per, sections // 2 * per), 0)
    dst = lax.broadcasted_iota(jnp.int32, src.shape, 1)
    at = (dst // per * nc + lax.axis_index("core")) * per + dst % per
    pick_core = jnp.where(src == at, 1.0, 0.0).astype(BF16)
    base = dot(hidden[last], out_grad, ((0,), (0,)))

    slopes = [slopes[s] for s in range(last)]
    ready = (pick_early, pick_late, pick_core, pick_even, pick_odd, gee_last, base)
    cuts = size(ROWS)
    piece = width // cuts
    cut = lax.axis_index(ROWS) * piece
    both, upper, cut, *ready = fence(both, upper, cut, *ready, *slopes)
    ready, slopes = ready[:-last], ready[-last:]
    rows_in, rows_out = fence(
        both[:, per:].reshape(units, width), both[:, :per].reshape(units, width)
    )

    gees, results = [], [upper]
    for s in reversed(range(last)):
        part = dot(upper, rows_out, ((1,), (1,))).astype(BF16)
        back = lax.all_gather(part, "mp").astype(F32).sum(0)
        gee = fence((back * slopes[s]).astype(BF16))
        gees.append(gee)
        branch = dot(gee, rows_in, ((1,), (0,))).astype(BF16)
        if s > 0:
            total = shared(branch, ROWS).astype(F32).sum(0)
            upper = fence((upper.astype(F32) + total).astype(BF16))
            results.append(upper)
        if s == 2:
            early = lax.all_gather(jnp.concatenate(results, 0), TOK, axis=0)
            early = early.reshape(groups * (last - 1) * each, width)

    second = lax.dynamic_slice_in_dim(
        upper, cut, piece, 1, allow_negative_indices=False
    )
    branch, second = fence(branch, second)
    total = exchange(branch.reshape(each, cuts, piece).transpose(1, 0, 2), ROWS)
    first = (second.astype(F32) + total.astype(F32).sum(0)).astype(BF16)
    *gees, second, first = fence(*gees, second, first)
    gees.append(gees[-1])
    gs = [jnp.concatenate(gees[q : q + 2], 0) for q in range(0, sections, 2)]
    gs = [g.reshape(2 * each, nz, nc * per).transpose(1, 0, 2) for g in gs]
    gs = jnp.concatenate(gs, 2)
    late = jnp.concatenate([second, first], 0)
    late = jnp.concatenate([jnp.broadcast_to(late[None], (nz,) + late.shape), gs], 2)
    late = exchange(late, "z")
    gs = late[:, :, piece:]
    late = shared(late[:, :, :piece], ROWS)
    left = lax.all_gather(late[: cuts // 2], "core", axis=0)
    right = lax.all_gather(jnp.concatenate([late[cuts // 2 :], gs[None]], 0), "core", axis=0)
    in_grads, grad_in, grad_out = finish(
        *ready,
        left.reshape(nc, cuts // 2, -1, piece),
        right.reshape(nc, cuts // 2 + 1, -1, piece),
        inputs.reshape(sections * tok_rows, width),
        early,
    )
    return (
        in_grads.reshape(1, tok_rows, width),
        grad_in.reshape(w_in.shape),
        grad_out.reshape(w_out.shape),
    )


def solution(mesh):
    split = Mesh(
        mesh.devices.reshape(
            mesh.shape["section"] // 2, 2, mesh.shape["dp"] // 2, 2, mesh.shape["mp"]
        ),
        ("x", "core", "z", "yl", "mp"),
    )
    placed = (
        P(SEC, None, "mp"),
        P(SEC, None, DP),
        P(None, "mp"),
        P(DP, SEC, None, "mp"),
        P(DP, SEC, None, "mp"),
    )
    return jax.shard_map(
        body,
        mesh=split,
        in_specs=placed,
        out_specs=(P(SEC, None, "mp"), P(DP, SEC, None, "mp"), P(DP, SEC, None, "mp")),
        check_vma=False,
    )
```

```python
import jax
import jax.numpy as jnp
from jax import lax
from jax.experimental import pallas as pl
from jax.experimental.pallas import tpu as pltpu
from jax.sharding import Mesh
from jax.sharding import PartitionSpec as P

F32 = jnp.float32
BF16 = jnp.bfloat16
LANES = 128
SEC = ("x", "core")
DP = ("z", "yl")
TOK = ("core", "z")
HID = ("z", "core")
ROWS = ("x", "yl")
PLANE = ("x", "yl", "core")


def size(axes):
    n = 1
    for a in axes:
        n *= lax.axis_size(a)
    return n


def exchange(value, axes):
    return lax.all_to_all(value, axes, 0, 0, tiled=True)


def shared(value, axes):
    n = size(axes)
    return exchange(jnp.broadcast_to(value[None], (n,) + value.shape), axes)


def fence(*values):
    return lax.optimization_barrier(values if len(values) > 1 else values[0])


def gelu_slope(value):
    cdf = 0.5 * (1.0 + lax.erf(value * 0.7071067811865476))
    dens = jnp.exp(-0.5 * value * value) * 0.3989422804014327
    return cdf + value * dens


def dot(left, right, dims):
    return lax.dot_general(left, right, (dims, ((), ())), preferred_element_type=F32)


def unpack_kernel(both, upper, rows_out, rows_in, part, sems):
    groups, two, width = both.shape
    per = two // 2
    cut = 4
    n = groups // cut

    def copy(w, i, ref):
        return pltpu.make_async_copy(
            both.at[pl.ds(i * n, n), pl.ds(w * per, per)],
            ref.at[pl.ds(i * n, n)],
            sems.at[w, i],
        )

    copies = [copy(0, i, rows_out) for i in range(cut)]
    others = [copy(1, i, rows_in) for i in range(cut)]
    for c in copies + others:
        c.start()
    for i, c in enumerate(copies):
        c.wait()
        rows = rows_out[i * n : (i + 1) * n].reshape(n * per, width)
        part[:, i * n * per : (i + 1) * n * per] = dot(
            upper[...], rows, ((1,), (1,))
        ).astype(BF16)
    for c in others:
        c.wait()


def unpack(both, upper):
    groups, two, width = both.shape
    local = pl.BlockSpec(memory_space=pltpu.VMEM)
    rows = jax.ShapeDtypeStruct((groups, two // 2, width), BF16)
    rows_out, rows_in, part = pl.pallas_call(
        unpack_kernel,
        in_specs=[pl.BlockSpec(memory_space=pltpu.MemorySpace.HBM), local],
        out_specs=[local] * 3,
        out_shape=[
            rows,
            rows,
            jax.ShapeDtypeStruct((upper.shape[0], groups * two // 2), BF16),
        ],
        scratch_shapes=[pltpu.SemaphoreType.DMA((2, 4))],
        compiler_params=pltpu.CompilerParams(vmem_limit_bytes=4 << 20),
        name="unpack",
    )(pltpu.with_memory_space_constraint(both, pltpu.HBM), upper)
    return rows_out.reshape(-1, width), rows_in.reshape(-1, width), part


def pack_kernel(*refs):
    *rows, out = refs
    out[...] = jnp.concatenate([r[...] for r in rows], 0)


def pack(rows):
    local = pl.BlockSpec(memory_space=pltpu.VMEM)
    shape = (len(rows) * rows[0].shape[0], rows[0].shape[1])
    return pl.pallas_call(
        pack_kernel,
        in_specs=[local] * len(rows),
        out_specs=local,
        out_shape=jax.ShapeDtypeStruct(shape, BF16),
        compiler_params=pltpu.CompilerParams(vmem_limit_bytes=2 << 20),
        name="pack",
    )(*rows)


def finish_kernel(
    pick_early, pick_late, pick_core, pick_even, pick_odd, gee_last, base, left, right, inputs, early,
    in_grads, grad_in, grad_out,
    x_buf, e_buf, even, odd, sems,
):
    tok_rows, block = in_grads.shape
    per = gee_last.shape[1]
    step, steps = pl.program_id(0), pl.num_programs(0)
    nc, half, rows, piece = left.shape

    def both_cores(value):
        return value.reshape(nc * rows, piece)

    def copies(i):
        cols = pl.ds(pl.multiple_of(i * block, block), block)
        return (
            pltpu.make_async_copy(inputs.at[:, cols], x_buf.at[i], sems.at[0, i]),
            pltpu.make_async_copy(early.at[:, cols], e_buf.at[i], sems.at[1, i]),
        )

    @pl.when(step == 0)
    def _():
        for i in range(x_buf.shape[0]):
            for copy in copies(i):
                copy.start()
        mine = dot(both_cores(right[:, half]), pick_core[...], ((1,), (0,))).astype(BF16)
        even[...] = dot(pick_even[...], mine, ((1,), (0,))).astype(BF16)
        odd[...] = dot(pick_odd[...], mine, ((1,), (0,))).astype(BF16)

    for copy in copies(step):
        copy.wait()
    at = block // piece * (step % (steps // 2))
    late = jnp.concatenate(
        [
            jnp.where(step < steps // 2, both_cores(left[:, at + i]), both_cores(right[:, at + i]))
            for i in range(block // piece)
        ],
        1,
    )
    x = x_buf[step]
    n = x.shape[0] // tok_rows


    def rows_of(s):
        return x[s * tok_rows : (s + 1) * tok_rows]

    total = dot(gee_last[...], rows_of(n - 1), ((0,), (0,)))
    for j in range(n - 1):
        gee = (even, odd)[j % 2][:, j // 2 * per : (j // 2 + 1) * per]
        total += dot(gee, rows_of(n - 2 - j), ((0,), (0,)))
    grad_in[...] = total
    found = dot(pick_early[...], e_buf[step], ((1,), (0,)))
    row = lax.broadcasted_iota(jnp.int32, late.shape, 0)
    second = jnp.where(row % 8 < 4, late.astype(F32), 0.0).astype(BF16)
    picked = dot(pick_late[:tok_rows], late, ((1,), (0,)))
    in_grads[...] = (found[:tok_rows] + picked).astype(BF16)
    grad_out[...] = (
        base[...] + found[tok_rows:] + dot(pick_late[tok_rows:], second, ((1,), (0,)))
    )


def finish(pick_early, pick_late, pick_core, pick_even, pick_odd, gee_last, base, left, right, inputs, early):
    per, width = base.shape
    tok_rows = gee_last.shape[0]
    steps = 4
    block = width // steps
    inputs = pltpu.with_memory_space_constraint(inputs, pltpu.HBM)
    early = pltpu.with_memory_space_constraint(early, pltpu.HBM)
    whole = lambda a: pl.BlockSpec(a.shape, lambda i: (0,) * a.ndim)
    cut = lambda rows: pl.BlockSpec((rows, block), lambda i: (0, i))
    return pl.pallas_call(
        finish_kernel,
        grid=(steps,),
        in_specs=[
            whole(pick_early),
            whole(pick_late),
            whole(pick_core),
            whole(pick_even),
            whole(pick_odd),
            whole(gee_last),
            cut(per),
            whole(left),
            whole(right),
            pl.BlockSpec(memory_space=pltpu.MemorySpace.HBM),
            pl.BlockSpec(memory_space=pltpu.MemorySpace.HBM),
        ],
        out_specs=[cut(tok_rows), cut(per), cut(per)],
        out_shape=[
            jax.ShapeDtypeStruct((tok_rows, width), BF16),
            jax.ShapeDtypeStruct((per, width), F32),
            jax.ShapeDtypeStruct((per, width), F32),
        ],
        scratch_shapes=[
            pltpu.VMEM((steps, inputs.shape[0], block), BF16),
            pltpu.VMEM((steps, early.shape[0], block), BF16),
            pltpu.VMEM((tok_rows, pick_core.shape[1]), BF16),
            pltpu.VMEM((tok_rows, pick_core.shape[1]), BF16),
            pltpu.SemaphoreType.DMA((2, steps)),
        ],
        compiler_params=pltpu.CompilerParams(vmem_limit_bytes=24 << 20),
        name="finish",
    )(pick_early, pick_late, pick_core, pick_even, pick_odd, gee_last, base, left, right, inputs, early)


def body(layer_inputs, pre_act, out_grad, w_in, w_out):
    nc, nz = lax.axis_size("core"), lax.axis_size("z")
    sections, groups = size(SEC), nz * nc
    tok_rows, width = out_grad.shape
    per = w_in.shape[2]
    each = tok_rows // groups
    units = groups * per
    last = sections - 1
    own_in = w_in.reshape(per, width)
    own_out = w_out.reshape(per, width)
    spot = lax.axis_index(SEC)
    mine = lax.axis_index(TOK)

    both = lax.all_gather(jnp.concatenate([own_out, own_in], 0), HID, axis=0)

    inputs = lax.all_gather(layer_inputs[0], SEC, axis=0)

    own_pre = exchange(
        pre_act[0].reshape(tok_rows, sections, per).transpose(1, 0, 2), SEC
    )
    part = dot(out_grad, own_out, ((1,), (1,))).astype(BF16)
    back = lax.all_gather(part, "mp").astype(F32).sum(0)
    gee_last = (back * gelu_slope(own_pre[last].astype(F32))).astype(BF16)
    cuts = size(PLANE)
    branch = dot(gee_last, own_in, ((1,), (0,))).astype(BF16)
    branch = exchange(branch.reshape(tok_rows, cuts, -1).transpose(1, 0, 2), PLANE)
    branch = branch.astype(F32).sum(0).astype(BF16).reshape(groups, 1, each, LANES)
    some = sections // lax.axis_size("mp")
    sent = lax.dynamic_slice_in_dim(own_pre, lax.axis_index("mp") * some, some, 0)
    sent = sent.reshape(some, groups, each * per // LANES, LANES).transpose(1, 2, 0, 3)
    sent = jnp.concatenate([branch, sent], 1)
    got = exchange(sent, TOK)
    branch = got[:, 0].reshape(nc, nz, each, LANES).astype(F32).sum(1).astype(BF16)
    branch = shared(branch.transpose(1, 0, 2).reshape(each, nc * LANES), ROWS)
    total = branch.transpose(1, 0, 2).reshape(each, width)
    pre = lax.all_gather(got[:, 1], "mp", axis=0)
    pre = pre.reshape(-1, nc, nz, some, each, per).transpose(0, 3, 4, 2, 1, 5)
    pre = pre.reshape(sections, each, units)[:last]
    slopes = gelu_slope(pre.reshape(last, each, units).astype(F32))
    upper = lax.dynamic_slice_in_dim(out_grad, mine * each, each, 0)
    upper = (upper.astype(F32) + total.astype(F32)).astype(BF16)
    hidden = jax.nn.gelu(own_pre.astype(F32), approximate=False).astype(BF16)
    hidden_rows = hidden[1:last].reshape(last - 1, groups, each, per)[::-1]
    hidden_rows = hidden_rows.transpose(3, 1, 0, 2).reshape(per, -1)
    token = lax.broadcasted_iota(jnp.int32, (tok_rows, hidden_rows.shape[1]), 0)
    col = lax.broadcasted_iota(jnp.int32, (tok_rows, hidden_rows.shape[1]), 1)
    at = token // each * ((last - 1) * each) + (last - spot) * each + token % each
    pick_early = jnp.where((col == at) & (spot > 1), 1.0, 0.0).astype(BF16)
    pick_early = jnp.concatenate([pick_early, hidden_rows], 0)
    token = lax.broadcasted_iota(jnp.int32, (tok_rows, 2 * tok_rows), 0)
    col = lax.broadcasted_iota(jnp.int32, (tok_rows, 2 * tok_rows), 1)
    at = token // each * (2 * each) + (1 - spot) * each + token % each
    pick_late = jnp.where((col == at) & (spot < 2), 1.0, 0.0).astype(BF16)
    hidden_late = hidden[0].T.reshape(per, groups, 1, each)
    hidden_late = jnp.pad(hidden_late, ((0, 0), (0, 0), (0, 1), (0, 0))).reshape(per, -1)
    pick_late = jnp.concatenate([pick_late, hidden_late], 0)
    at = token // each * (2 * each) + token % each
    pick_even = jnp.where(col == at, 1.0, 0.0).astype(BF16)
    pick_odd = jnp.where(col == at + each, 1.0, 0.0).astype(BF16)
    src = lax.broadcasted_iota(jnp.int32, (sections // 2 * nc * per, sections // 2 * per), 0)
    dst = lax.broadcasted_iota(jnp.int32, src.shape, 1)
    at = (dst // per * nc + lax.axis_index("core")) * per + dst % per
    pick_core = jnp.where(src == at, 1.0, 0.0).astype(BF16)
    base = dot(hidden[last], out_grad, ((0,), (0,)))

    slopes = [slopes[s] for s in range(last)]
    ready = (pick_early, pick_late, pick_core, pick_even, pick_odd, gee_last, base)
    cuts = size(ROWS)
    piece = width // cuts
    cut = lax.axis_index(ROWS) * piece
    both, upper, cut, *ready = fence(both, upper, cut, *ready, *slopes)
    ready, slopes = ready[:-last], ready[-last:]
    rows_out, rows_in, part = fence(*unpack(both, upper))

    gees, results = [], [upper]
    for s in reversed(range(last)):
        if s < last - 1:
            part = dot(upper, rows_out, ((1,), (1,))).astype(BF16)
        back = lax.all_gather(part, "mp").astype(F32).sum(0)
        gee = fence((back * slopes[s]).astype(BF16))
        gees.append(gee)
        branch = dot(gee, rows_in, ((1,), (0,))).astype(BF16)
        if s > 0:
            total = shared(branch, ROWS).astype(F32).sum(0)
            upper = fence((upper.astype(F32) + total).astype(BF16))
            results.append(upper)
        if s == 2:
            early = lax.all_gather(pack(results), TOK, axis=0)
            early = early.reshape(groups * (last - 1) * each, width)

    second = lax.dynamic_slice_in_dim(
        upper, cut, piece, 1, allow_negative_indices=False
    )
    branch, second = fence(branch, second)
    total = exchange(branch.reshape(each, cuts, piece).transpose(1, 0, 2), ROWS)
    first = (second.astype(F32) + total.astype(F32).sum(0)).astype(BF16)
    *gees, second, first = fence(*gees, second, first)
    gees.append(gees[-1])
    gs = [jnp.concatenate(gees[q : q + 2], 0) for q in range(0, sections, 2)]
    gs = [g.reshape(2 * each, nz, nc * per).transpose(1, 0, 2) for g in gs]
    gs = jnp.concatenate(gs, 2)
    late = jnp.concatenate([second, first], 0)
    late = jnp.concatenate([jnp.broadcast_to(late[None], (nz,) + late.shape), gs], 2)
    late = exchange(late, "z")
    gs = late[:, :, piece:]
    late = shared(late[:, :, :piece], ROWS)
    left = lax.all_gather(late[: cuts // 2], "core", axis=0)
    right = lax.all_gather(jnp.concatenate([late[cuts // 2 :], gs[None]], 0), "core", axis=0)
    in_grads, grad_in, grad_out = finish(
        *ready,
        left.reshape(nc, cuts // 2, -1, piece),
        right.reshape(nc, cuts // 2 + 1, -1, piece),
        inputs.reshape(sections * tok_rows, width),
        early,
    )
    return (
        in_grads.reshape(1, tok_rows, width),
        grad_in.reshape(w_in.shape),
        grad_out.reshape(w_out.shape),
    )


def solution(mesh):
    split = Mesh(
        mesh.devices.reshape(
            mesh.shape["section"] // 2, 2, mesh.shape["dp"] // 2, 2, mesh.shape["mp"]
        ),
        ("x", "core", "z", "yl", "mp"),
    )
    placed = (
        P(SEC, None, "mp"),
        P(SEC, None, DP),
        P(None, "mp"),
        P(DP, SEC, None, "mp"),
        P(DP, SEC, None, "mp"),
    )
    return jax.shard_map(
        body,
        mesh=split,
        in_specs=placed,
        out_specs=(P(SEC, None, "mp"), P(DP, SEC, None, "mp"), P(DP, SEC, None, "mp")),
        check_vma=False,
    )
```

```python
import jax
import jax.numpy as jnp
from jax import lax
from jax.experimental import pallas as pl
from jax.experimental.pallas import tpu as pltpu
from jax.sharding import Mesh
from jax.sharding import PartitionSpec as P

F32 = jnp.float32
BF16 = jnp.bfloat16
LANES = 128
SEC = ("x", "core")
DP = ("z", "yl")
TOK = ("core", "z")
HID = ("z", "core")
ROWS = ("x", "yl")
PLANE = ("x", "yl", "core")


def size(axes):
    n = 1
    for a in axes:
        n *= lax.axis_size(a)
    return n


def exchange(value, axes):
    return lax.all_to_all(value, axes, 0, 0, tiled=True)


def shared(value, axes):
    n = size(axes)
    return exchange(jnp.broadcast_to(value[None], (n,) + value.shape), axes)


def fence(*values):
    return lax.optimization_barrier(values if len(values) > 1 else values[0])


def gelu_slope(value):
    cdf = 0.5 * (1.0 + lax.erf(value * 0.7071067811865476))
    dens = jnp.exp(-0.5 * value * value) * 0.3989422804014327
    return cdf + value * dens


def dot(left, right, dims):
    return lax.dot_general(left, right, (dims, ((), ())), preferred_element_type=F32)


def unpack_kernel(both, upper, cols_out, rows_in, part, buf, sems):
    groups, two, width = both.shape
    per = two // 2
    cut = 4
    n = groups // cut

    def copy(w, i, ref):
        return pltpu.make_async_copy(
            both.at[pl.ds(i * n, n), pl.ds(w * per, per)],
            ref.at[pl.ds(i * n, n)],
            sems.at[w, i],
        )

    copies = [copy(0, i, buf) for i in range(cut)]
    others = [copy(1, i, rows_in) for i in range(cut)]
    for c in copies + others:
        c.start()
    for i, c in enumerate(copies):
        c.wait()
        at = slice(i * n * per, (i + 1) * n * per)
        cols = buf[i * n : (i + 1) * n].reshape(n * per, width).T
        cols_out[:, at] = cols
        part[:, at] = dot(upper[...], cols, ((1,), (0,))).astype(BF16)
    for c in others:
        c.wait()


def unpack(both, upper):
    groups, two, width = both.shape
    units = groups * two // 2
    local = pl.BlockSpec(memory_space=pltpu.VMEM)
    rows = (groups, two // 2, width)
    cols_out, rows_in, part = pl.pallas_call(
        unpack_kernel,
        in_specs=[pl.BlockSpec(memory_space=pltpu.MemorySpace.HBM), local],
        out_specs=[local] * 3,
        out_shape=[
            jax.ShapeDtypeStruct((width, units), BF16),
            jax.ShapeDtypeStruct(rows, BF16),
            jax.ShapeDtypeStruct((upper.shape[0], units), BF16),
        ],
        scratch_shapes=[pltpu.VMEM(rows, BF16), pltpu.SemaphoreType.DMA((2, 4))],
        compiler_params=pltpu.CompilerParams(vmem_limit_bytes=8 << 20),
        name="unpack",
    )(pltpu.with_memory_space_constraint(both, pltpu.HBM), upper)
    return cols_out, rows_in.reshape(units, width), part


def pack_kernel(*refs):
    *rows, out = refs
    out[...] = jnp.concatenate([r[...] for r in rows], 0)


def pack(rows):
    local = pl.BlockSpec(memory_space=pltpu.VMEM)
    shape = (len(rows) * rows[0].shape[0], rows[0].shape[1])
    return pl.pallas_call(
        pack_kernel,
        in_specs=[local] * len(rows),
        out_specs=local,
        out_shape=jax.ShapeDtypeStruct(shape, BF16),
        compiler_params=pltpu.CompilerParams(vmem_limit_bytes=2 << 20),
        name="pack",
    )(*rows)


def finish_kernel(
    pick_early, pick_late, pick_core, pick_even, pick_odd, gee_last, base, left, right, inputs, early,
    in_grads, grad_in, grad_out,
    x_buf, e_buf, even, odd, sems,
):
    tok_rows, block = in_grads.shape
    per = gee_last.shape[1]
    step, steps = pl.program_id(0), pl.num_programs(0)
    nc, half, rows, piece = left.shape

    def both_cores(value):
        return value.reshape(nc * rows, piece)

    def copies(i):
        cols = pl.ds(pl.multiple_of(i * block, block), block)
        return (
            pltpu.make_async_copy(inputs.at[:, cols], x_buf.at[i], sems.at[0, i]),
            pltpu.make_async_copy(early.at[:, cols], e_buf.at[i], sems.at[1, i]),
        )

    @pl.when(step == 0)
    def _():
        for i in range(x_buf.shape[0]):
            for copy in copies(i):
                copy.start()
        mine = dot(both_cores(right[:, half]), pick_core[...], ((1,), (0,))).astype(BF16)
        even[...] = dot(pick_even[...], mine, ((1,), (0,))).astype(BF16)
        odd[...] = dot(pick_odd[...], mine, ((1,), (0,))).astype(BF16)

    for copy in copies(step):
        copy.wait()
    at = block // piece * (step % (steps // 2))
    late = jnp.concatenate(
        [
            jnp.where(step < steps // 2, both_cores(left[:, at + i]), both_cores(right[:, at + i]))
            for i in range(block // piece)
        ],
        1,
    )
    x = x_buf[step]
    n = x.shape[0] // tok_rows


    def rows_of(s):
        return x[s * tok_rows : (s + 1) * tok_rows]

    total = dot(gee_last[...], rows_of(n - 1), ((0,), (0,)))
    for j in range(n - 1):
        gee = (even, odd)[j % 2][:, j // 2 * per : (j // 2 + 1) * per]
        total += dot(gee, rows_of(n - 2 - j), ((0,), (0,)))
    grad_in[...] = total
    found = dot(pick_early[...], e_buf[step], ((1,), (0,)))
    row = lax.broadcasted_iota(jnp.int32, late.shape, 0)
    second = jnp.where(row % 8 < 4, late.astype(F32), 0.0).astype(BF16)
    picked = dot(pick_late[:tok_rows], late, ((1,), (0,)))
    in_grads[...] = (found[:tok_rows] + picked).astype(BF16)
    grad_out[...] = (
        base[...] + found[tok_rows:] + dot(pick_late[tok_rows:], second, ((1,), (0,)))
    )


def finish(pick_early, pick_late, pick_core, pick_even, pick_odd, gee_last, base, left, right, inputs, early):
    per, width = base.shape
    tok_rows = gee_last.shape[0]
    steps = 4
    block = width // steps
    inputs = pltpu.with_memory_space_constraint(inputs, pltpu.HBM)
    early = pltpu.with_memory_space_constraint(early, pltpu.HBM)
    whole = lambda a: pl.BlockSpec(a.shape, lambda i: (0,) * a.ndim)
    cut = lambda rows: pl.BlockSpec((rows, block), lambda i: (0, i))
    return pl.pallas_call(
        finish_kernel,
        grid=(steps,),
        in_specs=[
            whole(pick_early),
            whole(pick_late),
            whole(pick_core),
            whole(pick_even),
            whole(pick_odd),
            whole(gee_last),
            cut(per),
            whole(left),
            whole(right),
            pl.BlockSpec(memory_space=pltpu.MemorySpace.HBM),
            pl.BlockSpec(memory_space=pltpu.MemorySpace.HBM),
        ],
        out_specs=[cut(tok_rows), cut(per), cut(per)],
        out_shape=[
            jax.ShapeDtypeStruct((tok_rows, width), BF16),
            jax.ShapeDtypeStruct((per, width), F32),
            jax.ShapeDtypeStruct((per, width), F32),
        ],
        scratch_shapes=[
            pltpu.VMEM((steps, inputs.shape[0], block), BF16),
            pltpu.VMEM((steps, early.shape[0], block), BF16),
            pltpu.VMEM((tok_rows, pick_core.shape[1]), BF16),
            pltpu.VMEM((tok_rows, pick_core.shape[1]), BF16),
            pltpu.SemaphoreType.DMA((2, steps)),
        ],
        compiler_params=pltpu.CompilerParams(vmem_limit_bytes=24 << 20),
        name="finish",
    )(pick_early, pick_late, pick_core, pick_even, pick_odd, gee_last, base, left, right, inputs, early)


def body(layer_inputs, pre_act, out_grad, w_in, w_out):
    nc, nz = lax.axis_size("core"), lax.axis_size("z")
    sections, groups = size(SEC), nz * nc
    tok_rows, width = out_grad.shape
    per = w_in.shape[2]
    each = tok_rows // groups
    units = groups * per
    last = sections - 1
    own_in = w_in.reshape(per, width)
    own_out = w_out.reshape(per, width)
    spot = lax.axis_index(SEC)
    mine = lax.axis_index(TOK)

    both = lax.all_gather(jnp.concatenate([own_out, own_in], 0), HID, axis=0)

    inputs = lax.all_gather(layer_inputs[0], SEC, axis=0)

    own_pre = exchange(
        pre_act[0].reshape(tok_rows, sections, per).transpose(1, 0, 2), SEC
    )
    part = dot(out_grad, own_out, ((1,), (1,))).astype(BF16)
    back = lax.all_gather(part, "mp").astype(F32).sum(0)
    gee_last = (back * gelu_slope(own_pre[last].astype(F32))).astype(BF16)
    cuts = size(PLANE)
    branch = dot(gee_last, own_in, ((1,), (0,))).astype(BF16)
    branch = exchange(branch.reshape(tok_rows, cuts, -1).transpose(1, 0, 2), PLANE)
    branch = branch.astype(F32).sum(0).astype(BF16).reshape(groups, 1, each, LANES)
    some = sections // lax.axis_size("mp")
    sent = lax.dynamic_slice_in_dim(own_pre, lax.axis_index("mp") * some, some, 0)
    sent = sent.reshape(some, groups, each * per // LANES, LANES).transpose(1, 2, 0, 3)
    sent = jnp.concatenate([branch, sent], 1)
    got = exchange(sent, TOK)
    branch = got[:, 0].reshape(nc, nz, each, LANES).astype(F32).sum(1).astype(BF16)
    branch = shared(branch.transpose(1, 0, 2).reshape(each, nc * LANES), ROWS)
    total = branch.transpose(1, 0, 2).reshape(each, width)
    pre = lax.all_gather(got[:, 1], "mp", axis=0)
    pre = pre.reshape(-1, nc, nz, some, each, per).transpose(0, 3, 4, 2, 1, 5)
    pre = pre.reshape(sections, each, units)[:last]
    slopes = gelu_slope(pre.reshape(last, each, units).astype(F32))
    upper = lax.dynamic_slice_in_dim(out_grad, mine * each, each, 0)
    upper = (upper.astype(F32) + total.astype(F32)).astype(BF16)
    hidden = jax.nn.gelu(own_pre.astype(F32), approximate=False).astype(BF16)
    hidden_rows = hidden[1:last].reshape(last - 1, groups, each, per)[::-1]
    hidden_rows = hidden_rows.transpose(3, 1, 0, 2).reshape(per, -1)
    token = lax.broadcasted_iota(jnp.int32, (tok_rows, hidden_rows.shape[1]), 0)
    col = lax.broadcasted_iota(jnp.int32, (tok_rows, hidden_rows.shape[1]), 1)
    at = token // each * ((last - 1) * each) + (last - spot) * each + token % each
    pick_early = jnp.where((col == at) & (spot > 1), 1.0, 0.0).astype(BF16)
    pick_early = jnp.concatenate([pick_early, hidden_rows], 0)
    token = lax.broadcasted_iota(jnp.int32, (tok_rows, 2 * tok_rows), 0)
    col = lax.broadcasted_iota(jnp.int32, (tok_rows, 2 * tok_rows), 1)
    at = token // each * (2 * each) + (1 - spot) * each + token % each
    pick_late = jnp.where((col == at) & (spot < 2), 1.0, 0.0).astype(BF16)
    hidden_late = hidden[0].T.reshape(per, groups, 1, each)
    hidden_late = jnp.pad(hidden_late, ((0, 0), (0, 0), (0, 1), (0, 0))).reshape(per, -1)
    pick_late = jnp.concatenate([pick_late, hidden_late], 0)
    at = token // each * (2 * each) + token % each
    pick_even = jnp.where(col == at, 1.0, 0.0).astype(BF16)
    pick_odd = jnp.where(col == at + each, 1.0, 0.0).astype(BF16)
    src = lax.broadcasted_iota(jnp.int32, (sections // 2 * nc * per, sections // 2 * per), 0)
    dst = lax.broadcasted_iota(jnp.int32, src.shape, 1)
    at = (dst // per * nc + lax.axis_index("core")) * per + dst % per
    pick_core = jnp.where(src == at, 1.0, 0.0).astype(BF16)
    base = dot(hidden[last], out_grad, ((0,), (0,)))

    slopes = [slopes[s] for s in range(last)]
    ready = (pick_early, pick_late, pick_core, pick_even, pick_odd, gee_last, base)
    cuts = size(ROWS)
    piece = width // cuts
    cut = lax.axis_index(ROWS) * piece
    both, upper, cut, *ready = fence(both, upper, cut, *ready, *slopes)
    ready, slopes = ready[:-last], ready[-last:]
    cols_out, rows_in, part = fence(*unpack(both, upper))

    gees, results = [], [upper]
    for s in reversed(range(last)):
        if s < last - 1:
            part = dot(upper, cols_out, ((1,), (0,))).astype(BF16)
        back = lax.all_gather(part, "mp").astype(F32).sum(0)
        gee = fence((back * slopes[s]).astype(BF16))
        gees.append(gee)
        branch = dot(gee, rows_in, ((1,), (0,))).astype(BF16)
        if s > 0:
            total = shared(branch, ROWS).astype(F32).sum(0)
            upper = fence((upper.astype(F32) + total).astype(BF16))
            results.append(upper)
        if s == 2:
            early = lax.all_gather(pack(results), TOK, axis=0)
            early = early.reshape(groups * (last - 1) * each, width)

    second = lax.dynamic_slice_in_dim(
        upper, cut, piece, 1, allow_negative_indices=False
    )
    branch, second = fence(branch, second)
    total = exchange(branch.reshape(each, cuts, piece).transpose(1, 0, 2), ROWS)
    first = (second.astype(F32) + total.astype(F32).sum(0)).astype(BF16)
    *gees, second, first = fence(*gees, second, first)
    gees.append(gees[-1])
    gs = [jnp.concatenate(gees[q : q + 2], 0) for q in range(0, sections, 2)]
    gs = [g.reshape(2 * each, nz, nc * per).transpose(1, 0, 2) for g in gs]
    gs = jnp.concatenate(gs, 2)
    late = jnp.concatenate([second, first], 0)
    late = jnp.concatenate([jnp.broadcast_to(late[None], (nz,) + late.shape), gs], 2)
    late = exchange(late, "z")
    gs = late[:, :, piece:]
    late = shared(late[:, :, :piece], ROWS)
    left = lax.all_gather(late[: cuts // 2], "core", axis=0)
    right = lax.all_gather(jnp.concatenate([late[cuts // 2 :], gs[None]], 0), "core", axis=0)
    in_grads, grad_in, grad_out = finish(
        *ready,
        left.reshape(nc, cuts // 2, -1, piece),
        right.reshape(nc, cuts // 2 + 1, -1, piece),
        inputs.reshape(sections * tok_rows, width),
        early,
    )
    return (
        in_grads.reshape(1, tok_rows, width),
        grad_in.reshape(w_in.shape),
        grad_out.reshape(w_out.shape),
    )


def solution(mesh):
    split = Mesh(
        mesh.devices.reshape(
            mesh.shape["section"] // 2, 2, mesh.shape["dp"] // 2, 2, mesh.shape["mp"]
        ),
        ("x", "core", "z", "yl", "mp"),
    )
    placed = (
        P(SEC, None, "mp"),
        P(SEC, None, DP),
        P(None, "mp"),
        P(DP, SEC, None, "mp"),
        P(DP, SEC, None, "mp"),
    )
    return jax.shard_map(
        body,
        mesh=split,
        in_specs=placed,
        out_specs=(P(SEC, None, "mp"), P(DP, SEC, None, "mp"), P(DP, SEC, None, "mp")),
        check_vma=False,
    )
```

```python
import jax
import jax.numpy as jnp
from jax import lax
from jax.experimental import pallas as pl
from jax.experimental.pallas import tpu as pltpu
from jax.sharding import Mesh
from jax.sharding import PartitionSpec as P

F32 = jnp.float32
BF16 = jnp.bfloat16
LANES = 128
PARTS = (2, 2)
SEC = ("x", "core")
DP = ("z", "yl")
TOK = ("core", "z")
HID = ("z", "core")
ROWS = ("x", "yl")
PLANE = ("x", "yl", "core")


def size(axes):
    n = 1
    for a in axes:
        n *= lax.axis_size(a)
    return n


def exchange(value, axes):
    return lax.all_to_all(value, axes, 0, 0, tiled=True)


def shared(value, axes):
    n = size(axes)
    return exchange(jnp.broadcast_to(value[None], (n,) + value.shape), axes)


def fence(*values):
    return lax.optimization_barrier(values if len(values) > 1 else values[0])


def gelu_slope(value):
    cdf = 0.5 * (1.0 + lax.erf(value * 0.7071067811865476))
    dens = jnp.exp(-0.5 * value * value) * 0.3989422804014327
    return cdf + value * dens


def dot(left, right, dims):
    return lax.dot_general(left, right, (dims, ((), ())), preferred_element_type=F32)


def unpack_kernel(both, upper, *refs):
    *cols_out, rows_in, part, buf, sems = refs
    groups, two, width = both.shape
    per = two // 2
    cut = sems.shape[1]
    n = groups // cut
    homes = [
        c.at[:, pl.ds(i * n * per, n * per)]
        for c in cols_out
        for i in range(c.shape[1] // (n * per))
    ]

    def copy(w, i, ref):
        return pltpu.make_async_copy(
            both.at[pl.ds(i * n, n), pl.ds(w * per, per)],
            ref.at[pl.ds(i * n, n)],
            sems.at[w, i],
        )

    copies = [copy(0, i, buf) for i in range(cut)]
    others = [copy(1, i, rows_in) for i in range(cut)]
    for c in copies + others:
        c.start()
    for i, c in enumerate(copies):
        c.wait()
        at = slice(i * n * per, (i + 1) * n * per)
        cols = buf[i * n : (i + 1) * n].reshape(n * per, width).T
        homes[i][...] = cols
        part[:, at] = dot(upper[...], cols, ((1,), (0,))).astype(BF16)
    for c in others:
        c.wait()


def unpack(both, upper):
    groups, two, width = both.shape
    units = groups * two // 2
    local = pl.BlockSpec(memory_space=pltpu.VMEM)
    rows = (groups, two // 2, width)
    cut = 4
    *cols_out, rows_in, part = pl.pallas_call(
        unpack_kernel,
        in_specs=[pl.BlockSpec(memory_space=pltpu.MemorySpace.HBM), local],
        out_specs=[local] * (len(PARTS) + 2),
        out_shape=[jax.ShapeDtypeStruct((width, units // cut * k), BF16) for k in PARTS]
        + [
            jax.ShapeDtypeStruct(rows, BF16),
            jax.ShapeDtypeStruct((upper.shape[0], units), BF16),
        ],
        scratch_shapes=[pltpu.VMEM(rows, BF16), pltpu.SemaphoreType.DMA((2, cut))],
        compiler_params=pltpu.CompilerParams(vmem_limit_bytes=8 << 20),
        name="unpack",
    )(pltpu.with_memory_space_constraint(both, pltpu.HBM), upper)
    return (*cols_out, rows_in.reshape(units, width), part)


def product_kernel(parts, upper, *refs):
    *cols, total, part = refs
    total[...] = (upper[...].astype(F32) + parts[...].astype(F32).sum(0)).astype(BF16)
    at = 0
    for c in cols:
        n = c.shape[1]
        part[:, at : at + n] = dot(total[...], c[...], ((1,), (0,))).astype(BF16)
        at += n


def product(parts, upper, cols):
    local = pl.BlockSpec(memory_space=pltpu.VMEM)
    units = sum(c.shape[1] for c in cols)
    return pl.pallas_call(
        product_kernel,
        in_specs=[local] * (2 + len(cols)),
        out_specs=[local] * 2,
        out_shape=[
            jax.ShapeDtypeStruct(upper.shape, BF16),
            jax.ShapeDtypeStruct((upper.shape[0], units), BF16),
        ],
        compiler_params=pltpu.CompilerParams(vmem_limit_bytes=1 << 20),
        name="product",
    )(parts, upper, *cols)


def pack_kernel(*refs):
    *rows, out = refs
    out[...] = jnp.concatenate([r[...] for r in rows], 0)


def pack(rows):
    local = pl.BlockSpec(memory_space=pltpu.VMEM)
    shape = (len(rows) * rows[0].shape[0], rows[0].shape[1])
    return pl.pallas_call(
        pack_kernel,
        in_specs=[local] * len(rows),
        out_specs=local,
        out_shape=jax.ShapeDtypeStruct(shape, BF16),
        compiler_params=pltpu.CompilerParams(vmem_limit_bytes=2 << 20),
        name="pack",
    )(*rows)


def finish_kernel(
    pick_early, pick_late, pick_core, pick_even, pick_odd, gee_last, base, left, right, inputs, early,
    in_grads, grad_in, grad_out,
    x_buf, e_buf, even, odd, sems,
):
    tok_rows, block = in_grads.shape
    per = gee_last.shape[1]
    step, steps = pl.program_id(0), pl.num_programs(0)
    nc, half, rows, piece = left.shape

    def both_cores(value):
        return value.reshape(nc * rows, piece)

    def copies(i):
        cols = pl.ds(pl.multiple_of(i * block, block), block)
        return (
            pltpu.make_async_copy(inputs.at[:, cols], x_buf.at[i], sems.at[0, i]),
            pltpu.make_async_copy(early.at[:, cols], e_buf.at[i], sems.at[1, i]),
        )

    @pl.when(step == 0)
    def _():
        for i in range(x_buf.shape[0]):
            for copy in copies(i):
                copy.start()
        mine = dot(both_cores(right[:, half]), pick_core[...], ((1,), (0,))).astype(BF16)
        even[...] = dot(pick_even[...], mine, ((1,), (0,))).astype(BF16)
        odd[...] = dot(pick_odd[...], mine, ((1,), (0,))).astype(BF16)

    for copy in copies(step):
        copy.wait()
    at = block // piece * (step % (steps // 2))
    late = jnp.concatenate(
        [
            jnp.where(step < steps // 2, both_cores(left[:, at + i]), both_cores(right[:, at + i]))
            for i in range(block // piece)
        ],
        1,
    )
    x = x_buf[step]
    n = x.shape[0] // tok_rows


    def rows_of(s):
        return x[s * tok_rows : (s + 1) * tok_rows]

    total = dot(gee_last[...], rows_of(n - 1), ((0,), (0,)))
    for j in range(n - 1):
        gee = (even, odd)[j % 2][:, j // 2 * per : (j // 2 + 1) * per]
        total += dot(gee, rows_of(n - 2 - j), ((0,), (0,)))
    grad_in[...] = total
    found = dot(pick_early[...], e_buf[step], ((1,), (0,)))
    row = lax.broadcasted_iota(jnp.int32, late.shape, 0)
    second = jnp.where(row % 8 < 4, late.astype(F32), 0.0).astype(BF16)
    picked = dot(pick_late[:tok_rows], late, ((1,), (0,)))
    in_grads[...] = (found[:tok_rows] + picked).astype(BF16)
    grad_out[...] = (
        base[...] + found[tok_rows:] + dot(pick_late[tok_rows:], second, ((1,), (0,)))
    )


def finish(pick_early, pick_late, pick_core, pick_even, pick_odd, gee_last, base, left, right, inputs, early):
    per, width = base.shape
    tok_rows = gee_last.shape[0]
    steps = 4
    block = width // steps
    inputs = pltpu.with_memory_space_constraint(inputs, pltpu.HBM)
    early = pltpu.with_memory_space_constraint(early, pltpu.HBM)
    whole = lambda a: pl.BlockSpec(a.shape, lambda i: (0,) * a.ndim)
    cut = lambda rows: pl.BlockSpec((rows, block), lambda i: (0, i))
    return pl.pallas_call(
        finish_kernel,
        grid=(steps,),
        in_specs=[
            whole(pick_early),
            whole(pick_late),
            whole(pick_core),
            whole(pick_even),
            whole(pick_odd),
            whole(gee_last),
            cut(per),
            whole(left),
            whole(right),
            pl.BlockSpec(memory_space=pltpu.MemorySpace.HBM),
            pl.BlockSpec(memory_space=pltpu.MemorySpace.HBM),
        ],
        out_specs=[cut(tok_rows), cut(per), cut(per)],
        out_shape=[
            jax.ShapeDtypeStruct((tok_rows, width), BF16),
            jax.ShapeDtypeStruct((per, width), F32),
            jax.ShapeDtypeStruct((per, width), F32),
        ],
        scratch_shapes=[
            pltpu.VMEM((steps, inputs.shape[0], block), BF16),
            pltpu.VMEM((steps, early.shape[0], block), BF16),
            pltpu.VMEM((tok_rows, pick_core.shape[1]), BF16),
            pltpu.VMEM((tok_rows, pick_core.shape[1]), BF16),
            pltpu.SemaphoreType.DMA((2, steps)),
        ],
        compiler_params=pltpu.CompilerParams(vmem_limit_bytes=24 << 20),
        name="finish",
    )(pick_early, pick_late, pick_core, pick_even, pick_odd, gee_last, base, left, right, inputs, early)


def body(layer_inputs, pre_act, out_grad, w_in, w_out):
    nc, nz = lax.axis_size("core"), lax.axis_size("z")
    sections, groups = size(SEC), nz * nc
    tok_rows, width = out_grad.shape
    per = w_in.shape[2]
    each = tok_rows // groups
    units = groups * per
    last = sections - 1
    own_in = w_in.reshape(per, width)
    own_out = w_out.reshape(per, width)
    spot = lax.axis_index(SEC)
    mine = lax.axis_index(TOK)

    both = lax.all_gather(jnp.concatenate([own_out, own_in], 0), HID, axis=0)

    inputs = lax.all_gather(layer_inputs[0], SEC, axis=0)

    own_pre = exchange(
        pre_act[0].reshape(tok_rows, sections, per).transpose(1, 0, 2), SEC
    )
    part = dot(out_grad, own_out, ((1,), (1,))).astype(BF16)
    back = lax.all_gather(part, "mp").astype(F32).sum(0)
    gee_last = (back * gelu_slope(own_pre[last].astype(F32))).astype(BF16)
    cuts = size(PLANE)
    branch = dot(gee_last, own_in, ((1,), (0,))).astype(BF16)
    branch = exchange(branch.reshape(tok_rows, cuts, -1).transpose(1, 0, 2), PLANE)
    branch = branch.astype(F32).sum(0).astype(BF16).reshape(groups, 1, each, LANES)
    some = sections // lax.axis_size("mp")
    sent = lax.dynamic_slice_in_dim(own_pre, lax.axis_index("mp") * some, some, 0)
    sent = sent.reshape(some, groups, each * per // LANES, LANES).transpose(1, 2, 0, 3)
    sent = jnp.concatenate([branch, sent], 1)
    got = exchange(sent, TOK)
    branch = got[:, 0].reshape(nc, nz, each, LANES).astype(F32).sum(1).astype(BF16)
    branch = shared(branch.transpose(1, 0, 2).reshape(each, nc * LANES), ROWS)
    total = branch.transpose(1, 0, 2).reshape(each, width)
    pre = lax.all_gather(got[:, 1], "mp", axis=0)
    pre = pre.reshape(-1, nc, nz, some, each, per).transpose(0, 3, 4, 2, 1, 5)
    pre = pre.reshape(sections, each, units)[:last]
    slopes = gelu_slope(pre.reshape(last, each, units).astype(F32))
    upper = lax.dynamic_slice_in_dim(out_grad, mine * each, each, 0)
    upper = (upper.astype(F32) + total.astype(F32)).astype(BF16)
    hidden = jax.nn.gelu(own_pre.astype(F32), approximate=False).astype(BF16)
    hidden_rows = hidden[1:last].reshape(last - 1, groups, each, per)[::-1]
    hidden_rows = hidden_rows.transpose(3, 1, 0, 2).reshape(per, -1)
    token = lax.broadcasted_iota(jnp.int32, (tok_rows, hidden_rows.shape[1]), 0)
    col = lax.broadcasted_iota(jnp.int32, (tok_rows, hidden_rows.shape[1]), 1)
    at = token // each * ((last - 1) * each) + (last - spot) * each + token % each
    pick_early = jnp.where((col == at) & (spot > 1), 1.0, 0.0).astype(BF16)
    pick_early = jnp.concatenate([pick_early, hidden_rows], 0)
    token = lax.broadcasted_iota(jnp.int32, (tok_rows, 2 * tok_rows), 0)
    col = lax.broadcasted_iota(jnp.int32, (tok_rows, 2 * tok_rows), 1)
    at = token // each * (2 * each) + (1 - spot) * each + token % each
    pick_late = jnp.where((col == at) & (spot < 2), 1.0, 0.0).astype(BF16)
    hidden_late = hidden[0].T.reshape(per, groups, 1, each)
    hidden_late = jnp.pad(hidden_late, ((0, 0), (0, 0), (0, 1), (0, 0))).reshape(per, -1)
    pick_late = jnp.concatenate([pick_late, hidden_late], 0)
    at = token // each * (2 * each) + token % each
    pick_even = jnp.where(col == at, 1.0, 0.0).astype(BF16)
    pick_odd = jnp.where(col == at + each, 1.0, 0.0).astype(BF16)
    src = lax.broadcasted_iota(jnp.int32, (sections // 2 * nc * per, sections // 2 * per), 0)
    dst = lax.broadcasted_iota(jnp.int32, src.shape, 1)
    at = (dst // per * nc + lax.axis_index("core")) * per + dst % per
    pick_core = jnp.where(src == at, 1.0, 0.0).astype(BF16)
    base = dot(hidden[last], out_grad, ((0,), (0,)))

    slopes = [slopes[s] for s in range(last)]
    ready = (pick_early, pick_late, pick_core, pick_even, pick_odd, gee_last, base)
    cuts = size(ROWS)
    piece = width // cuts
    cut = lax.axis_index(ROWS) * piece
    both, upper, cut, *ready = fence(both, upper, cut, *ready, *slopes)
    ready, slopes = ready[:-last], ready[-last:]
    *cols_out, rows_in, part = fence(*unpack(both, upper))

    gees, results = [], [upper]
    for s in reversed(range(last)):
        back = lax.all_gather(part, "mp").astype(F32).sum(0)
        gee = fence((back * slopes[s]).astype(BF16))
        gees.append(gee)
        branch = dot(gee, rows_in, ((1,), (0,))).astype(BF16)
        if s == 2:
            parts = shared(branch, ROWS)
            upper = (upper.astype(F32) + parts.astype(F32).sum(0)).astype(BF16)
            results.append(fence(upper))
            early = lax.all_gather(pack(results), TOK, axis=0)
            early = early.reshape(groups * (last - 1) * each, width)
            upper, part = fence(*product(parts, results[-2], cols_out))
        elif s > 0:
            upper, part = fence(*product(shared(branch, ROWS), upper, cols_out))
            results.append(upper)

    second = lax.dynamic_slice_in_dim(
        upper, cut, piece, 1, allow_negative_indices=False
    )
    branch, second = fence(branch, second)
    total = exchange(branch.reshape(each, cuts, piece).transpose(1, 0, 2), ROWS)
    first = (second.astype(F32) + total.astype(F32).sum(0)).astype(BF16)
    *gees, second, first = fence(*gees, second, first)
    gees.append(gees[-1])
    gs = [jnp.concatenate(gees[q : q + 2], 0) for q in range(0, sections, 2)]
    gs = [g.reshape(2 * each, nz, nc * per).transpose(1, 0, 2) for g in gs]
    gs = jnp.concatenate(gs, 2)
    late = jnp.concatenate([second, first], 0)
    late = jnp.concatenate([jnp.broadcast_to(late[None], (nz,) + late.shape), gs], 2)
    late = exchange(late, "z")
    gs = late[:, :, piece:]
    late = shared(late[:, :, :piece], ROWS)
    left = lax.all_gather(late[: cuts // 2], "core", axis=0)
    right = lax.all_gather(jnp.concatenate([late[cuts // 2 :], gs[None]], 0), "core", axis=0)
    in_grads, grad_in, grad_out = finish(
        *ready,
        left.reshape(nc, cuts // 2, -1, piece),
        right.reshape(nc, cuts // 2 + 1, -1, piece),
        inputs.reshape(sections * tok_rows, width),
        early,
    )
    return (
        in_grads.reshape(1, tok_rows, width),
        grad_in.reshape(w_in.shape),
        grad_out.reshape(w_out.shape),
    )


def solution(mesh):
    split = Mesh(
        mesh.devices.reshape(
            mesh.shape["section"] // 2, 2, mesh.shape["dp"] // 2, 2, mesh.shape["mp"]
        ),
        ("x", "core", "z", "yl", "mp"),
    )
    placed = (
        P(SEC, None, "mp"),
        P(SEC, None, DP),
        P(None, "mp"),
        P(DP, SEC, None, "mp"),
        P(DP, SEC, None, "mp"),
    )
    return jax.shard_map(
        body,
        mesh=split,
        in_specs=placed,
        out_specs=(P(SEC, None, "mp"), P(DP, SEC, None, "mp"), P(DP, SEC, None, "mp")),
        check_vma=False,
    )
```

```python
import jax
import jax.numpy as jnp
from jax import lax
from jax.experimental import pallas as pl
from jax.experimental.pallas import tpu as pltpu
from jax.sharding import Mesh
from jax.sharding import PartitionSpec as P

F32 = jnp.float32
BF16 = jnp.bfloat16
LANES = 128
PARTS = (2, 2)
SEC = ("x", "core")
DP = ("z", "yl")
TOK = ("core", "z")
HID = ("z", "core")
ROWS = ("x", "yl")
PLANE = ("x", "yl", "core")


def size(axes):
    n = 1
    for a in axes:
        n *= lax.axis_size(a)
    return n


def exchange(value, axes):
    return lax.all_to_all(value, axes, 0, 0, tiled=True)


def shared(value, axes):
    n = size(axes)
    return exchange(jnp.broadcast_to(value[None], (n,) + value.shape), axes)


def fence(*values):
    return lax.optimization_barrier(values if len(values) > 1 else values[0])


def gelu_slope(value):
    cdf = 0.5 * (1.0 + lax.erf(value * 0.7071067811865476))
    dens = jnp.exp(-0.5 * value * value) * 0.3989422804014327
    return cdf + value * dens


def dot(left, right, dims):
    return lax.dot_general(left, right, (dims, ((), ())), preferred_element_type=F32)


def unpack_kernel(both, upper, *refs):
    *cols_out, rows_in, part, buf, sems = refs
    groups, two, width = both.shape
    per = two // 2
    cut = sems.shape[1]
    n = groups // cut
    homes = [
        c.at[:, pl.ds(i * n * per, n * per)]
        for c in cols_out
        for i in range(c.shape[1] // (n * per))
    ]

    def copy(w, i, ref):
        return pltpu.make_async_copy(
            both.at[pl.ds(i * n, n), pl.ds(w * per, per)],
            ref.at[pl.ds(i * n, n)],
            sems.at[w, i],
        )

    copies = [copy(0, i, buf) for i in range(cut)]
    others = [copy(1, i, rows_in) for i in range(cut)]
    for c in copies + others:
        c.start()
    for i, c in enumerate(copies):
        c.wait()
        at = slice(i * n * per, (i + 1) * n * per)
        cols = buf[i * n : (i + 1) * n].reshape(n * per, width).T
        homes[i][...] = cols
        part[:, at] = dot(upper[...], cols, ((1,), (0,))).astype(BF16)
    for c in others:
        c.wait()


def unpack(both, upper):
    groups, two, width = both.shape
    units = groups * two // 2
    local = pl.BlockSpec(memory_space=pltpu.VMEM)
    rows = (groups, two // 2, width)
    cut = 4
    *cols_out, rows_in, part = pl.pallas_call(
        unpack_kernel,
        in_specs=[pl.BlockSpec(memory_space=pltpu.MemorySpace.HBM), local],
        out_specs=[local] * (len(PARTS) + 2),
        out_shape=[jax.ShapeDtypeStruct((width, units // cut * k), BF16) for k in PARTS]
        + [
            jax.ShapeDtypeStruct(rows, BF16),
            jax.ShapeDtypeStruct((upper.shape[0], units), BF16),
        ],
        scratch_shapes=[pltpu.VMEM(rows, BF16), pltpu.SemaphoreType.DMA((2, cut))],
        compiler_params=pltpu.CompilerParams(vmem_limit_bytes=8 << 20),
        name="unpack",
    )(pltpu.with_memory_space_constraint(both, pltpu.HBM), upper)
    return (*cols_out, rows_in.reshape(units, width), part)


def product_kernel(parts, upper, *refs):
    *cols, total, part = refs
    total[...] = (upper[...].astype(F32) + parts[...].astype(F32).sum(0)).astype(BF16)
    at = 0
    for c in cols:
        n = c.shape[1]
        part[:, at : at + n] = dot(total[...], c[...], ((1,), (0,))).astype(BF16)
        at += n


def product(parts, upper, cols):
    local = pl.BlockSpec(memory_space=pltpu.VMEM)
    units = sum(c.shape[1] for c in cols)
    return pl.pallas_call(
        product_kernel,
        in_specs=[local] * (2 + len(cols)),
        out_specs=[local] * 2,
        out_shape=[
            jax.ShapeDtypeStruct(upper.shape, BF16),
            jax.ShapeDtypeStruct((upper.shape[0], units), BF16),
        ],
        compiler_params=pltpu.CompilerParams(vmem_limit_bytes=1 << 20),
        name="product",
    )(parts, upper, *cols)


def second_product_kernel(backs, slope, rows, gee, sent):
    value = (backs[0].astype(F32) + backs[1].astype(F32)) * slope[...]
    gee[...] = value.astype(BF16)
    branch = dot(gee[...], rows[...], ((1,), (0,))).astype(BF16)
    n = sent.shape[2]
    for i in range(sent.shape[0]):
        at = i * n % branch.shape[1]
        sent[i] = branch[:, at : at + n]


def second_product(backs, slope, rows, copies, width):
    local = pl.BlockSpec(memory_space=pltpu.VMEM)
    return pl.pallas_call(
        second_product_kernel,
        in_specs=[local] * 3,
        out_specs=[local] * 2,
        out_shape=[
            jax.ShapeDtypeStruct(slope.shape, BF16),
            jax.ShapeDtypeStruct((copies, slope.shape[0], width), BF16),
        ],
        compiler_params=pltpu.CompilerParams(vmem_limit_bytes=1 << 20),
        name="second_product",
    )(backs, slope, rows)


def pack_kernel(*refs):
    *rows, out = refs
    out[...] = jnp.concatenate([r[...] for r in rows], 0)


def pack(rows):
    local = pl.BlockSpec(memory_space=pltpu.VMEM)
    shape = (len(rows) * rows[0].shape[0], rows[0].shape[1])
    return pl.pallas_call(
        pack_kernel,
        in_specs=[local] * len(rows),
        out_specs=local,
        out_shape=jax.ShapeDtypeStruct(shape, BF16),
        compiler_params=pltpu.CompilerParams(vmem_limit_bytes=2 << 20),
        name="pack",
    )(*rows)


def build_kernel(parts, second, *refs):
    *gees, out = refs
    nz, rows, wide = out.shape
    first = second[...].astype(F32) + parts[...].astype(F32).sum(0)
    late = jnp.concatenate([second[...].astype(F32), first], 0)
    piece = late.shape[1]
    n = gees[0].shape[1] // nz
    pairs = []
    for q in range((wide - piece) // n):
        pair = gees[2 * q : 2 * q + 2]
        pairs.append(jnp.concatenate([g[...].astype(F32) for g in (pair + pair)[:2]], 0))
    for z in range(nz):
        own = [p[:, z * n : (z + 1) * n] for p in pairs]
        out[z] = jnp.concatenate([late] + own, 1).astype(BF16)


def build(parts, second, gees, planes):
    local = pl.BlockSpec(memory_space=pltpu.VMEM)
    each, piece = second.shape
    wide = piece + (len(gees) + 1) // 2 * gees[0].shape[1] // planes
    return pl.pallas_call(
        build_kernel,
        in_specs=[local] * (2 + len(gees)),
        out_specs=local,
        out_shape=jax.ShapeDtypeStruct((planes, 2 * each, wide), BF16),
        compiler_params=pltpu.CompilerParams(vmem_limit_bytes=4 << 20),
        name="build",
    )(parts, second, *gees)


def finish_kernel(
    pick_early, pick_late, pick_core, pick_even, pick_odd, gee_last, base, left, right, inputs, early,
    in_grads, grad_in, grad_out,
    x_buf, e_buf, even, odd, sems,
):
    tok_rows, block = in_grads.shape
    per = gee_last.shape[1]
    step, steps = pl.program_id(0), pl.num_programs(0)
    nc, half, rows, piece = left.shape

    def both_cores(value):
        return value.reshape(nc * rows, piece)

    def copies(i):
        cols = pl.ds(pl.multiple_of(i * block, block), block)
        return (
            pltpu.make_async_copy(inputs.at[:, cols], x_buf.at[i], sems.at[0, i]),
            pltpu.make_async_copy(early.at[:, cols], e_buf.at[i], sems.at[1, i]),
        )

    @pl.when(step == 0)
    def _():
        for i in range(x_buf.shape[0]):
            for copy in copies(i):
                copy.start()
        mine = dot(both_cores(right[:, half]), pick_core[...], ((1,), (0,))).astype(BF16)
        even[...] = dot(pick_even[...], mine, ((1,), (0,))).astype(BF16)
        odd[...] = dot(pick_odd[...], mine, ((1,), (0,))).astype(BF16)

    for copy in copies(step):
        copy.wait()
    at = block // piece * (step % (steps // 2))
    late = jnp.concatenate(
        [
            jnp.where(step < steps // 2, both_cores(left[:, at + i]), both_cores(right[:, at + i]))
            for i in range(block // piece)
        ],
        1,
    )
    x = x_buf[step]
    n = x.shape[0] // tok_rows


    def rows_of(s):
        return x[s * tok_rows : (s + 1) * tok_rows]

    total = dot(gee_last[...], rows_of(n - 1), ((0,), (0,)))
    for j in range(n - 1):
        gee = (even, odd)[j % 2][:, j // 2 * per : (j // 2 + 1) * per]
        total += dot(gee, rows_of(n - 2 - j), ((0,), (0,)))
    grad_in[...] = total
    found = dot(pick_early[...], e_buf[step], ((1,), (0,)))
    row = lax.broadcasted_iota(jnp.int32, late.shape, 0)
    second = jnp.where(row % 8 < 4, late.astype(F32), 0.0).astype(BF16)
    picked = dot(pick_late[:tok_rows], late, ((1,), (0,)))
    in_grads[...] = (found[:tok_rows] + picked).astype(BF16)
    grad_out[...] = (
        base[...] + found[tok_rows:] + dot(pick_late[tok_rows:], second, ((1,), (0,)))
    )


def finish(pick_early, pick_late, pick_core, pick_even, pick_odd, gee_last, base, left, right, inputs, early):
    per, width = base.shape
    tok_rows = gee_last.shape[0]
    steps = 4
    block = width // steps
    inputs = pltpu.with_memory_space_constraint(inputs, pltpu.HBM)
    early = pltpu.with_memory_space_constraint(early, pltpu.HBM)
    whole = lambda a: pl.BlockSpec(a.shape, lambda i: (0,) * a.ndim)
    cut = lambda rows: pl.BlockSpec((rows, block), lambda i: (0, i))
    return pl.pallas_call(
        finish_kernel,
        grid=(steps,),
        in_specs=[
            whole(pick_early),
            whole(pick_late),
            whole(pick_core),
            whole(pick_even),
            whole(pick_odd),
            whole(gee_last),
            cut(per),
            whole(left),
            whole(right),
            pl.BlockSpec(memory_space=pltpu.MemorySpace.HBM),
            pl.BlockSpec(memory_space=pltpu.MemorySpace.HBM),
        ],
        out_specs=[cut(tok_rows), cut(per), cut(per)],
        out_shape=[
            jax.ShapeDtypeStruct((tok_rows, width), BF16),
            jax.ShapeDtypeStruct((per, width), F32),
            jax.ShapeDtypeStruct((per, width), F32),
        ],
        scratch_shapes=[
            pltpu.VMEM((steps, inputs.shape[0], block), BF16),
            pltpu.VMEM((steps, early.shape[0], block), BF16),
            pltpu.VMEM((tok_rows, pick_core.shape[1]), BF16),
            pltpu.VMEM((tok_rows, pick_core.shape[1]), BF16),
            pltpu.SemaphoreType.DMA((2, steps)),
        ],
        compiler_params=pltpu.CompilerParams(vmem_limit_bytes=24 << 20),
        name="finish",
    )(pick_early, pick_late, pick_core, pick_even, pick_odd, gee_last, base, left, right, inputs, early)


def body(layer_inputs, pre_act, out_grad, w_in, w_out):
    nc, nz = lax.axis_size("core"), lax.axis_size("z")
    sections, groups = size(SEC), nz * nc
    tok_rows, width = out_grad.shape
    per = w_in.shape[2]
    each = tok_rows // groups
    units = groups * per
    last = sections - 1
    own_in = w_in.reshape(per, width)
    own_out = w_out.reshape(per, width)
    spot = lax.axis_index(SEC)
    mine = lax.axis_index(TOK)

    both = lax.all_gather(jnp.concatenate([own_out, own_in], 0), HID, axis=0)

    inputs = lax.all_gather(layer_inputs[0], SEC, axis=0)

    own_pre = exchange(
        pre_act[0].reshape(tok_rows, sections, per).transpose(1, 0, 2), SEC
    )
    part = dot(out_grad, own_out, ((1,), (1,))).astype(BF16)
    back = lax.all_gather(part, "mp").astype(F32).sum(0)
    gee_last = (back * gelu_slope(own_pre[last].astype(F32))).astype(BF16)
    cuts = size(PLANE)
    branch = dot(gee_last, own_in, ((1,), (0,))).astype(BF16)
    branch = exchange(branch.reshape(tok_rows, cuts, -1).transpose(1, 0, 2), PLANE)
    branch = branch.astype(F32).sum(0).astype(BF16).reshape(groups, 1, each, LANES)
    some = sections // lax.axis_size("mp")
    sent = lax.dynamic_slice_in_dim(own_pre, lax.axis_index("mp") * some, some, 0)
    sent = sent.reshape(some, groups, each * per // LANES, LANES).transpose(1, 2, 0, 3)
    sent = jnp.concatenate([branch, sent], 1)
    got = exchange(sent, TOK)
    branch = got[:, 0].reshape(nc, nz, each, LANES).astype(F32).sum(1).astype(BF16)
    branch = shared(branch.transpose(1, 0, 2).reshape(each, nc * LANES), ROWS)
    total = branch.transpose(1, 0, 2).reshape(each, width)
    pre = lax.all_gather(got[:, 1], "mp", axis=0)
    pre = pre.reshape(-1, nc, nz, some, each, per).transpose(0, 3, 4, 2, 1, 5)
    pre = pre.reshape(sections, each, units)[:last]
    slopes = gelu_slope(pre.reshape(last, each, units).astype(F32))
    upper = lax.dynamic_slice_in_dim(out_grad, mine * each, each, 0)
    upper = (upper.astype(F32) + total.astype(F32)).astype(BF16)
    hidden = jax.nn.gelu(own_pre.astype(F32), approximate=False).astype(BF16)
    hidden_rows = hidden[1:last].reshape(last - 1, groups, each, per)[::-1]
    hidden_rows = hidden_rows.transpose(3, 1, 0, 2).reshape(per, -1)
    token = lax.broadcasted_iota(jnp.int32, (tok_rows, hidden_rows.shape[1]), 0)
    col = lax.broadcasted_iota(jnp.int32, (tok_rows, hidden_rows.shape[1]), 1)
    at = token // each * ((last - 1) * each) + (last - spot) * each + token % each
    pick_early = jnp.where((col == at) & (spot > 1), 1.0, 0.0).astype(BF16)
    pick_early = jnp.concatenate([pick_early, hidden_rows], 0)
    token = lax.broadcasted_iota(jnp.int32, (tok_rows, 2 * tok_rows), 0)
    col = lax.broadcasted_iota(jnp.int32, (tok_rows, 2 * tok_rows), 1)
    at = token // each * (2 * each) + (1 - spot) * each + token % each
    pick_late = jnp.where((col == at) & (spot < 2), 1.0, 0.0).astype(BF16)
    hidden_late = hidden[0].T.reshape(per, groups, 1, each)
    hidden_late = jnp.pad(hidden_late, ((0, 0), (0, 0), (0, 1), (0, 0))).reshape(per, -1)
    pick_late = jnp.concatenate([pick_late, hidden_late], 0)
    at = token // each * (2 * each) + token % each
    pick_even = jnp.where(col == at, 1.0, 0.0).astype(BF16)
    pick_odd = jnp.where(col == at + each, 1.0, 0.0).astype(BF16)
    src = lax.broadcasted_iota(jnp.int32, (sections // 2 * nc * per, sections // 2 * per), 0)
    dst = lax.broadcasted_iota(jnp.int32, src.shape, 1)
    at = (dst // per * nc + lax.axis_index("core")) * per + dst % per
    pick_core = jnp.where(src == at, 1.0, 0.0).astype(BF16)
    base = dot(hidden[last], out_grad, ((0,), (0,)))

    slopes = [slopes[s] for s in range(last)]
    ready = (pick_early, pick_late, pick_core, pick_even, pick_odd, gee_last, base)
    cuts = size(ROWS)
    piece = width // cuts
    cut = lax.axis_index(ROWS) * piece
    both, upper, cut, *ready = fence(both, upper, cut, *ready, *slopes)
    ready, slopes = ready[:-last], ready[-last:]
    *cols_out, rows_in, part = fence(*unpack(both, upper))

    gees, results = [], [upper]
    for s in reversed(range(last)):
        backs = lax.all_gather(part, "mp")
        gee, sent = fence(
            *second_product(backs, slopes[s], rows_in, cuts, width if s > 0 else piece)
        )
        gees.append(gee)
        if s == 2:
            parts = exchange(sent, ROWS)
            upper = (upper.astype(F32) + parts.astype(F32).sum(0)).astype(BF16)
            results.append(fence(upper))
            early = lax.all_gather(pack(results), TOK, axis=0)
            early = early.reshape(groups * (last - 1) * each, width)
            upper, part = fence(*product(parts, results[-2], cols_out))
        elif s > 0:
            upper, part = fence(*product(exchange(sent, ROWS), upper, cols_out))
            results.append(upper)

    second = lax.dynamic_slice_in_dim(
        upper, cut, piece, 1, allow_negative_indices=False
    )
    sent, second = fence(sent, second)
    total = exchange(sent, ROWS)
    late = build(total, second, gees, nz)
    late = exchange(late, "z")
    gs = late[:, :, piece:]
    late = shared(late[:, :, :piece], ROWS)
    left = lax.all_gather(late[: cuts // 2], "core", axis=0)
    right = lax.all_gather(jnp.concatenate([late[cuts // 2 :], gs[None]], 0), "core", axis=0)
    in_grads, grad_in, grad_out = finish(
        *ready,
        left.reshape(nc, cuts // 2, -1, piece),
        right.reshape(nc, cuts // 2 + 1, -1, piece),
        inputs.reshape(sections * tok_rows, width),
        early,
    )
    return (
        in_grads.reshape(1, tok_rows, width),
        grad_in.reshape(w_in.shape),
        grad_out.reshape(w_out.shape),
    )


def solution(mesh):
    split = Mesh(
        mesh.devices.reshape(
            mesh.shape["section"] // 2, 2, mesh.shape["dp"] // 2, 2, mesh.shape["mp"]
        ),
        ("x", "core", "z", "yl", "mp"),
    )
    placed = (
        P(SEC, None, "mp"),
        P(SEC, None, DP),
        P(None, "mp"),
        P(DP, SEC, None, "mp"),
        P(DP, SEC, None, "mp"),
    )
    return jax.shard_map(
        body,
        mesh=split,
        in_specs=placed,
        out_specs=(P(SEC, None, "mp"), P(DP, SEC, None, "mp"), P(DP, SEC, None, "mp")),
        check_vma=False,
    )
```

```python
import jax
import jax.numpy as jnp
from jax import lax
from jax.experimental import pallas as pl
from jax.experimental.pallas import tpu as pltpu
from jax.sharding import Mesh
from jax.sharding import PartitionSpec as P

F32 = jnp.float32
BF16 = jnp.bfloat16
LANES = 128
PARTS = (2, 2)
SEC = ("x", "core")
DP = ("z", "yl")
TOK = ("core", "z")
HID = ("z", "core")
ROWS = ("x", "yl")
PLANE = ("x", "yl", "core")


def size(axes):
    n = 1
    for a in axes:
        n *= lax.axis_size(a)
    return n


def exchange(value, axes):
    return lax.all_to_all(value, axes, 0, 0, tiled=True)


def shared(value, axes):
    n = size(axes)
    return exchange(jnp.broadcast_to(value[None], (n,) + value.shape), axes)


def fence(*values):
    return lax.optimization_barrier(values if len(values) > 1 else values[0])


def gelu_slope(value):
    cdf = 0.5 * (1.0 + lax.erf(value * 0.7071067811865476))
    dens = jnp.exp(-0.5 * value * value) * 0.3989422804014327
    return cdf + value * dens


def dot(left, right, dims):
    return lax.dot_general(left, right, (dims, ((), ())), preferred_element_type=F32)


def unpack_kernel(both, upper, *refs):
    *cols_out, rows_in, part, buf, sems = refs
    groups, two, width = both.shape
    per = two // 2
    cut = sems.shape[1]
    n = groups // cut
    homes = [
        c.at[:, pl.ds(i * n * per, n * per)]
        for c in cols_out
        for i in range(c.shape[1] // (n * per))
    ]

    def copy(w, i, ref):
        return pltpu.make_async_copy(
            both.at[pl.ds(i * n, n), pl.ds(w * per, per)],
            ref.at[pl.ds(i * n, n)],
            sems.at[w, i],
        )

    copies = [copy(0, i, buf) for i in range(cut)]
    others = [copy(1, i, rows_in) for i in range(cut)]
    for c in copies + others:
        c.start()
    for i, c in enumerate(copies):
        c.wait()
        at = slice(i * n * per, (i + 1) * n * per)
        cols = buf[i * n : (i + 1) * n].reshape(n * per, width).T
        homes[i][...] = cols
        part[:, at] = dot(upper[...], cols, ((1,), (0,))).astype(BF16)
    for c in others:
        c.wait()


def unpack(both, upper):
    groups, two, width = both.shape
    units = groups * two // 2
    local = pl.BlockSpec(memory_space=pltpu.VMEM)
    rows = (groups, two // 2, width)
    cut = 4
    *cols_out, rows_in, part = pl.pallas_call(
        unpack_kernel,
        in_specs=[pl.BlockSpec(memory_space=pltpu.MemorySpace.HBM), local],
        out_specs=[local] * (len(PARTS) + 2),
        out_shape=[jax.ShapeDtypeStruct((width, units // cut * k), BF16) for k in PARTS]
        + [
            jax.ShapeDtypeStruct(rows, BF16),
            jax.ShapeDtypeStruct((upper.shape[0], units), BF16),
        ],
        scratch_shapes=[pltpu.VMEM(rows, BF16), pltpu.SemaphoreType.DMA((2, cut))],
        compiler_params=pltpu.CompilerParams(vmem_limit_bytes=8 << 20),
        name="unpack",
    )(pltpu.with_memory_space_constraint(both, pltpu.HBM), upper)
    return (*cols_out, rows_in.reshape(units, width), part)


def product_kernel(parts, upper, *refs):
    *cols, total, part = refs
    total[...] = (upper[...].astype(F32) + parts[...].astype(F32).sum(0)).astype(BF16)
    at = 0
    for c in cols:
        n = c.shape[1]
        part[:, at : at + n] = dot(total[...], c[...], ((1,), (0,))).astype(BF16)
        at += n


def product(parts, upper, cols):
    local = pl.BlockSpec(memory_space=pltpu.VMEM)
    units = sum(c.shape[1] for c in cols)
    return pl.pallas_call(
        product_kernel,
        in_specs=[local] * (2 + len(cols)),
        out_specs=[local] * 2,
        out_shape=[
            jax.ShapeDtypeStruct(upper.shape, BF16),
            jax.ShapeDtypeStruct((upper.shape[0], units), BF16),
        ],
        compiler_params=pltpu.CompilerParams(vmem_limit_bytes=1 << 20),
        name="product",
    )(parts, upper, *cols)


def second_product_kernel(backs, slope, rows, gee, sent):
    value = (backs[0].astype(F32) + backs[1].astype(F32)) * slope[...]
    gee[...] = value.astype(BF16)
    branch = dot(gee[...], rows[...], ((1,), (0,))).astype(BF16)
    n = sent.shape[2]
    for i in range(sent.shape[0]):
        at = i * n % branch.shape[1]
        sent[i] = branch[:, at : at + n]


def second_product(backs, slope, rows, copies, width):
    local = pl.BlockSpec(memory_space=pltpu.VMEM)
    return pl.pallas_call(
        second_product_kernel,
        in_specs=[local] * 3,
        out_specs=[local] * 2,
        out_shape=[
            jax.ShapeDtypeStruct(slope.shape, BF16),
            jax.ShapeDtypeStruct((copies, slope.shape[0], width), BF16),
        ],
        compiler_params=pltpu.CompilerParams(vmem_limit_bytes=1 << 20),
        name="second_product",
    )(backs, slope, rows)


def pack_kernel(*refs):
    *rows, out = refs
    out[...] = jnp.concatenate([r[...] for r in rows], 0)


def pack(rows):
    local = pl.BlockSpec(memory_space=pltpu.VMEM)
    shape = (len(rows) * rows[0].shape[0], rows[0].shape[1])
    return pl.pallas_call(
        pack_kernel,
        in_specs=[local] * len(rows),
        out_specs=local,
        out_shape=jax.ShapeDtypeStruct(shape, BF16),
        compiler_params=pltpu.CompilerParams(vmem_limit_bytes=2 << 20),
        name="pack",
    )(*rows)


def build_kernel(parts, second, *refs):
    *gees, out = refs
    nz, rows, wide = out.shape
    first = second[...].astype(F32) + parts[...].astype(F32).sum(0)
    late = jnp.concatenate([second[...].astype(F32), first], 0)
    piece = late.shape[1]
    n = gees[0].shape[1] // nz
    pairs = []
    for q in range((wide - piece) // n):
        pair = gees[2 * q : 2 * q + 2]
        pairs.append(jnp.concatenate([g[...].astype(F32) for g in (pair + pair)[:2]], 0))
    for z in range(nz):
        own = [p[:, z * n : (z + 1) * n] for p in pairs]
        out[z] = jnp.concatenate([late] + own, 1).astype(BF16)


def build(parts, second, gees, planes):
    local = pl.BlockSpec(memory_space=pltpu.VMEM)
    each, piece = second.shape
    wide = piece + (len(gees) + 1) // 2 * gees[0].shape[1] // planes
    return pl.pallas_call(
        build_kernel,
        in_specs=[local] * (2 + len(gees)),
        out_specs=local,
        out_shape=jax.ShapeDtypeStruct((planes, 2 * each, wide), BF16),
        compiler_params=pltpu.CompilerParams(vmem_limit_bytes=4 << 20),
        name="build",
    )(parts, second, *gees)


def finish_kernel(
    place, rows_early, rows_late, gee_last, base, left, right, inputs, early,
    in_grads, grad_in, grad_out,
    x_buf, e_buf, gees, pick_early, pick_late, sems,
):
    tok_rows, block = in_grads.shape
    per = gee_last.shape[1]
    step, steps = pl.program_id(0), pl.num_programs(0)
    nc, half, rows, piece = left.shape

    def both_cores(value):
        return value.reshape(nc * rows, piece)

    n = inputs.shape[1] * nc // tok_rows
    each = tok_rows // inputs.shape[0]
    bits = each.bit_length() - 1

    def pick(shape, width, first, fits=None):
        token = lax.broadcasted_iota(jnp.int32, shape, 0)
        col = lax.broadcasted_iota(jnp.int32, shape, 1)
        hit = col == (token >> bits) * width + first + (token & (each - 1))
        hit = hit if fits is None else hit & fits
        return jnp.where(hit, 1.0, 0.0).astype(BF16)

    part = block // inputs.shape[2]

    def copies(i):
        cols = pl.ds(pl.multiple_of(i * block, block), block)
        planes = inputs.shape[0] // nc
        yield pltpu.make_async_copy(early.at[:, cols], e_buf.at[i], sems.at[nc, i])
        for c in range(nc):
            yield pltpu.make_async_copy(
                inputs.at[pl.ds(c * planes + i * part, part)], x_buf.at[i, c], sems.at[c, i]
            )

    @pl.when(step == 0)
    def _():
        for i in range(x_buf.shape[0]):
            for copy in copies(i):
                copy.start()
        spot, core = place[0:1, 0:1], place[1:2, 0:1]
        pick_early[:tok_rows] = pick(
            (tok_rows, rows_early.shape[1]), (n - 2) * each, (n - 1 - spot) * each, spot > 1
        )
        pick_early[tok_rows:] = rows_early[...]
        pick_late[:tok_rows] = pick(
            (tok_rows, rows_late.shape[1]), 2 * each, (1 - spot) * each, spot < 2
        )
        pick_late[tok_rows:] = rows_late[...]
        shape = (piece, piece // nc)
        src = lax.broadcasted_iota(jnp.int32, shape, 0)
        dst = lax.broadcasted_iota(jnp.int32, shape, 1)
        low = per.bit_length() - 1
        own_core = src == ((dst >> low) * nc + core) * per + (dst & (per - 1))
        pick_core = jnp.where(own_core, 1.0, 0.0).astype(BF16)
        mine = dot(both_cores(right[:, half]), pick_core, ((1,), (0,))).astype(BF16)
        own = {n - 1: gee_last[...]}
        for j in range(2):
            found = dot(pick((tok_rows, nc * rows), 2 * each, j * each), mine, ((1,), (0,))).astype(BF16)
            for s in range(n - 2 - j, -1, -2):
                q = (n - 2 - j - s) // 2
                own[s] = found[:, q * per : (q + 1) * per]
        few = tok_rows // nc
        for c in range(nc):
            gees[c] = jnp.concatenate([own[s][c * few : (c + 1) * few] for s in range(n)], 0)

    for copy in copies(step):
        copy.wait()
    at = block // piece * (step % (steps // 2))
    late = jnp.concatenate(
        [
            jnp.where(step < steps // 2, both_cores(left[:, at + i]), both_cores(right[:, at + i]))
            for i in range(block // piece)
        ],
        1,
    )
    total = jnp.zeros(grad_in.shape, F32)
    for c in range(nc):
        x = jnp.concatenate([x_buf[step, c, k] for k in range(part)], 1)
        total += dot(gees[c], x, ((0,), (0,)))
    grad_in[...] = total
    found = dot(pick_early[...], e_buf[step], ((1,), (0,)))
    row = lax.broadcasted_iota(jnp.int32, late.shape, 0)
    second = jnp.where(row % 8 < 4, late.astype(F32), 0.0).astype(BF16)
    picked = dot(pick_late[:tok_rows], late, ((1,), (0,)))
    in_grads[...] = (found[:tok_rows] + picked).astype(BF16)
    grad_out[...] = (
        base[...] + found[tok_rows:] + dot(pick_late[tok_rows:], second, ((1,), (0,)))
    )


def finish(place, rows_early, rows_late, gee_last, base, left, right, inputs, early):
    per, width = base.shape
    tok_rows, nc = gee_last.shape[0], left.shape[0]
    steps = 4
    block = width // steps
    inputs = pltpu.with_memory_space_constraint(inputs, pltpu.HBM)
    early = pltpu.with_memory_space_constraint(early, pltpu.HBM)
    whole = lambda a: pl.BlockSpec(a.shape, lambda i: (0,) * a.ndim)
    cut = lambda rows: pl.BlockSpec((rows, block), lambda i: (0, i))
    return pl.pallas_call(
        finish_kernel,
        grid=(steps,),
        in_specs=[
            whole(place),
            whole(rows_early),
            whole(rows_late),
            whole(gee_last),
            cut(per),
            whole(left),
            whole(right),
            pl.BlockSpec(memory_space=pltpu.MemorySpace.HBM),
            pl.BlockSpec(memory_space=pltpu.MemorySpace.HBM),
        ],
        out_specs=[cut(tok_rows), cut(per), cut(per)],
        out_shape=[
            jax.ShapeDtypeStruct((tok_rows, width), BF16),
            jax.ShapeDtypeStruct((per, width), F32),
            jax.ShapeDtypeStruct((per, width), F32),
        ],
        scratch_shapes=[
            pltpu.VMEM((steps, nc, block // inputs.shape[2], *inputs.shape[1:]), BF16),
            pltpu.VMEM((steps, early.shape[0], block), BF16),
            pltpu.VMEM((nc, inputs.shape[1], per), BF16),
            pltpu.VMEM((tok_rows + per, rows_early.shape[1]), BF16),
            pltpu.VMEM((tok_rows + per, rows_late.shape[1]), BF16),
            pltpu.SemaphoreType.DMA((nc + 1, steps)),
        ],
        compiler_params=pltpu.CompilerParams(vmem_limit_bytes=24 << 20),
        name="finish",
    )(place, rows_early, rows_late, gee_last, base, left, right, inputs, early)


def body(layer_inputs, pre_act, out_grad, w_in, w_out):
    nc, nz = lax.axis_size("core"), lax.axis_size("z")
    sections, groups = size(SEC), nz * nc
    tok_rows, width = out_grad.shape
    per = w_in.shape[2]
    each = tok_rows // groups
    units = groups * per
    last = sections - 1
    own_in = w_in.reshape(per, width)
    own_out = w_out.reshape(per, width)
    spot = lax.axis_index(SEC)
    mine = lax.axis_index(TOK)

    both = lax.all_gather(jnp.concatenate([own_out, own_in], 0), HID, axis=0)

    own_pre = exchange(
        pre_act[0].reshape(tok_rows, sections, per).transpose(1, 0, 2), SEC
    )
    part = dot(out_grad, own_out, ((1,), (1,))).astype(BF16)
    back = lax.all_gather(part, "mp").astype(F32).sum(0)
    gee_last = (back * gelu_slope(own_pre[last].astype(F32))).astype(BF16)
    cuts = size(PLANE)
    branch = dot(gee_last, own_in, ((1,), (0,))).astype(BF16)
    branch = exchange(branch.reshape(tok_rows, cuts, -1).transpose(1, 0, 2), PLANE)
    branch = branch.astype(F32).sum(0).astype(BF16).reshape(groups, 1, each, LANES)
    some = sections // lax.axis_size("mp")
    sent = lax.dynamic_slice_in_dim(own_pre, lax.axis_index("mp") * some, some, 0)
    sent = sent.reshape(some, groups, each * per // LANES, LANES).transpose(1, 2, 0, 3)
    sent = jnp.concatenate([branch, sent], 1)
    hidden = jax.nn.gelu(own_pre.astype(F32), approximate=False).astype(BF16)
    hidden_rows = hidden[1:last].reshape(last - 1, groups, each, per)[::-1]
    hidden_rows = hidden_rows.transpose(3, 1, 0, 2).reshape(per, -1)
    hidden_late = hidden[0].T.reshape(per, groups, 1, each)
    hidden_late = jnp.pad(hidden_late, ((0, 0), (0, 0), (0, 1), (0, 0))).reshape(per, -1)
    place = jnp.stack([jnp.full((LANES,), spot), jnp.full((LANES,), lax.axis_index("core"))])
    base = dot(hidden[last], out_grad, ((0,), (0,)))

    ready = (place, pack([hidden_rows]), pack([hidden_late]), gee_last, base)
    got = exchange(sent, TOK)
    got, *ready = fence(got, *ready)
    branch = got[:, 0].reshape(nc, nz, each, LANES).astype(F32).sum(1).astype(BF16)
    branch = shared(branch.transpose(1, 0, 2).reshape(each, nc * LANES), ROWS)
    total = branch.transpose(1, 0, 2).reshape(each, width)
    pre = lax.all_gather(got[:, 1], "mp", axis=0)
    pre = pre.reshape(-1, nc, nz, some, each, per).transpose(0, 3, 4, 2, 1, 5)
    pre = pre.reshape(sections, each, units)[:last]
    inputs, total, pre = fence(layer_inputs[0], total, pre)
    inputs = lax.dynamic_slice_in_dim(
        inputs, lax.axis_index("z") * (width // nz), width // nz, 1, allow_negative_indices=False
    )
    inputs = jnp.broadcast_to(
        inputs.reshape(1, nc, tok_rows // nc, width // nz),
        (sections // nc, nc, tok_rows // nc, width // nz),
    )
    inputs = exchange(inputs.reshape(sections, tok_rows // nc, width // nz), SEC)
    slopes = gelu_slope(pre.reshape(last, each, units).astype(F32))
    upper = lax.dynamic_slice_in_dim(out_grad, mine * each, each, 0)
    upper = (upper.astype(F32) + total.astype(F32)).astype(BF16)
    slopes = [slopes[s] for s in range(last)]
    cuts = size(ROWS)
    piece = width // cuts
    cut = lax.axis_index(ROWS) * piece
    inputs = lax.all_gather(inputs.reshape(-1, width // nz), TOK, axis=0)
    both, upper, cut, *ready = fence(both, upper, cut, *ready, *slopes)
    ready, slopes = ready[:-last], ready[-last:]
    *cols_out, rows_in, part = fence(*unpack(both, upper))

    gees, results = [], [upper]
    for s in reversed(range(last)):
        backs = lax.all_gather(part, "mp")
        gee, sent = fence(
            *second_product(backs, slopes[s], rows_in, cuts, width if s > 0 else piece)
        )
        gees.append(gee)
        if s == 2:
            parts = exchange(sent, ROWS)
            upper = (upper.astype(F32) + parts.astype(F32).sum(0)).astype(BF16)
            results.append(fence(upper))
            early = lax.all_gather(pack(results), TOK, axis=0)
            early = early.reshape(groups * (last - 1) * each, width)
            upper, part = fence(*product(parts, results[-2], cols_out))
        elif s > 0:
            upper, part = fence(*product(exchange(sent, ROWS), upper, cols_out))
            results.append(upper)

    second = lax.dynamic_slice_in_dim(
        upper, cut, piece, 1, allow_negative_indices=False
    )
    sent, second = fence(sent, second)
    total = exchange(sent, ROWS)
    late = build(total, second, gees, nz)
    late = exchange(late, "z")
    gs = late[:, :, piece:]
    late = shared(late[:, :, :piece], ROWS)
    left = lax.all_gather(late[: cuts // 2], "core", axis=0)
    right = lax.all_gather(jnp.concatenate([late[cuts // 2 :], gs[None]], 0), "core", axis=0)
    in_grads, grad_in, grad_out = finish(
        *ready,
        left.reshape(nc, cuts // 2, -1, piece),
        right.reshape(nc, cuts // 2 + 1, -1, piece),
        inputs,
        early,
    )
    return (
        in_grads.reshape(1, tok_rows, width),
        grad_in.reshape(w_in.shape),
        grad_out.reshape(w_out.shape),
    )


def solution(mesh):
    split = Mesh(
        mesh.devices.reshape(
            mesh.shape["section"] // 2, 2, mesh.shape["dp"] // 2, 2, mesh.shape["mp"]
        ),
        ("x", "core", "z", "yl", "mp"),
    )
    placed = (
        P(SEC, None, "mp"),
        P(SEC, None, DP),
        P(None, "mp"),
        P(DP, SEC, None, "mp"),
        P(DP, SEC, None, "mp"),
    )
    return jax.shard_map(
        body,
        mesh=split,
        in_specs=placed,
        out_specs=(P(SEC, None, "mp"), P(DP, SEC, None, "mp"), P(DP, SEC, None, "mp")),
        check_vma=False,
    )
```

```python
import jax
import jax.numpy as jnp
from jax import lax
from jax.experimental import pallas as pl
from jax.experimental.pallas import tpu as pltpu
from jax.sharding import Mesh
from jax.sharding import PartitionSpec as P

F32 = jnp.float32
BF16 = jnp.bfloat16
LANES = 128
PARTS = (2, 2)
SEC = ("x", "core")
DP = ("z", "yl")
TOK = ("core", "z")
HID = ("z", "core")
ROWS = ("x", "yl")
PLANE = ("x", "yl", "core")


def size(axes):
    n = 1
    for a in axes:
        n *= lax.axis_size(a)
    return n


def exchange(value, axes):
    return lax.all_to_all(value, axes, 0, 0, tiled=True)


def shared(value, axes):
    n = size(axes)
    return exchange(jnp.broadcast_to(value[None], (n,) + value.shape), axes)


def fence(*values):
    return lax.optimization_barrier(values if len(values) > 1 else values[0])


def gelu_slope(value):
    cdf = 0.5 * (1.0 + lax.erf(value * 0.7071067811865476))
    dens = jnp.exp(-0.5 * value * value) * 0.3989422804014327
    return cdf + value * dens


def dot(left, right, dims):
    return lax.dot_general(left, right, (dims, ((), ())), preferred_element_type=F32)


def unpack_kernel(both, upper, *refs):
    *cols_out, rows_in, part, buf, sems = refs
    groups, two, width = both.shape
    per = two // 2
    cut = sems.shape[1]
    n = groups // cut
    homes = [
        c.at[:, pl.ds(i * n * per, n * per)]
        for c in cols_out
        for i in range(c.shape[1] // (n * per))
    ]

    def copy(w, i, ref):
        return pltpu.make_async_copy(
            both.at[pl.ds(i * n, n), pl.ds(w * per, per)],
            ref.at[pl.ds(i * n, n)],
            sems.at[w, i],
        )

    copies = [copy(0, i, buf) for i in range(cut)]
    others = [copy(1, i, rows_in) for i in range(cut)]
    for c in copies + others:
        c.start()
    for i, c in enumerate(copies):
        c.wait()
        at = slice(i * n * per, (i + 1) * n * per)
        cols = buf[i * n : (i + 1) * n].reshape(n * per, width).T
        homes[i][...] = cols
        part[:, at] = dot(upper[...], cols, ((1,), (0,))).astype(BF16)
    for c in others:
        c.wait()


def unpack(both, upper):
    groups, two, width = both.shape
    units = groups * two // 2
    local = pl.BlockSpec(memory_space=pltpu.VMEM)
    rows = (groups, two // 2, width)
    cut = 4
    *cols_out, rows_in, part = pl.pallas_call(
        unpack_kernel,
        in_specs=[pl.BlockSpec(memory_space=pltpu.MemorySpace.HBM), local],
        out_specs=[local] * (len(PARTS) + 2),
        out_shape=[jax.ShapeDtypeStruct((width, units // cut * k), BF16) for k in PARTS]
        + [
            jax.ShapeDtypeStruct(rows, BF16),
            jax.ShapeDtypeStruct((upper.shape[0], units), BF16),
        ],
        scratch_shapes=[pltpu.VMEM(rows, BF16), pltpu.SemaphoreType.DMA((2, cut))],
        compiler_params=pltpu.CompilerParams(vmem_limit_bytes=8 << 20),
        name="unpack",
    )(pltpu.with_memory_space_constraint(both, pltpu.HBM), upper)
    return (*cols_out, rows_in.reshape(units, width), part)


def product_kernel(parts, upper, *refs):
    *cols, total, part = refs
    total[...] = (upper[...].astype(F32) + parts[...].astype(F32).sum(0)).astype(BF16)
    at = 0
    for c in cols:
        n = c.shape[1]
        part[:, at : at + n] = dot(total[...], c[...], ((1,), (0,))).astype(BF16)
        at += n


def product(parts, upper, cols):
    local = pl.BlockSpec(memory_space=pltpu.VMEM)
    units = sum(c.shape[1] for c in cols)
    return pl.pallas_call(
        product_kernel,
        in_specs=[local] * (2 + len(cols)),
        out_specs=[local] * 2,
        out_shape=[
            jax.ShapeDtypeStruct(upper.shape, BF16),
            jax.ShapeDtypeStruct((upper.shape[0], units), BF16),
        ],
        compiler_params=pltpu.CompilerParams(vmem_limit_bytes=1 << 20),
        name="product",
    )(parts, upper, *cols)


def reading_product_kernel(parts, upper, near, far, total, part, buf, sems):
    cut = sems.shape[0]
    n = far.shape[0] // cut
    copies = [
        pltpu.make_async_copy(far.at[pl.ds(i * n, n)], buf.at[pl.ds(i * n, n)], sems.at[i])
        for i in range(cut)
    ]
    for copy in copies:
        copy.start()
    total[...] = (upper[...].astype(F32) + parts[...].astype(F32).sum(0)).astype(BF16)
    units = near.shape[1]
    part[:, :units] = dot(total[...], near[...], ((1,), (0,))).astype(BF16)
    value = jnp.zeros((upper.shape[0], far.shape[1]), F32)
    for i, copy in enumerate(copies):
        copy.wait()
        at = slice(i * n, (i + 1) * n)
        value += dot(total[:, at], buf[at], ((1,), (0,)))
    part[:, units:] = value.astype(BF16)


def reading_product(parts, upper, near, far):
    local = pl.BlockSpec(memory_space=pltpu.VMEM)
    units = near.shape[1] + far.shape[1]
    return pl.pallas_call(
        reading_product_kernel,
        in_specs=[local] * 3 + [pl.BlockSpec(memory_space=pltpu.MemorySpace.HBM)],
        out_specs=[local] * 3,
        out_shape=[
            jax.ShapeDtypeStruct(upper.shape, BF16),
            jax.ShapeDtypeStruct((upper.shape[0], units), BF16),
            jax.ShapeDtypeStruct(far.shape, BF16),
        ],
        scratch_shapes=[pltpu.SemaphoreType.DMA((4,))],
        compiler_params=pltpu.CompilerParams(vmem_limit_bytes=4 << 20),
        name="reading_product",
    )(parts, upper, near, pltpu.with_memory_space_constraint(far, pltpu.HBM))


def second_product_kernel(backs, slope, rows, gee, sent):
    value = (backs[0].astype(F32) + backs[1].astype(F32)) * slope[...]
    gee[...] = value.astype(BF16)
    branch = dot(gee[...], rows[...], ((1,), (0,))).astype(BF16)
    n = sent.shape[2]
    for i in range(sent.shape[0]):
        at = i * n % branch.shape[1]
        sent[i] = branch[:, at : at + n]


def second_product(backs, slope, rows, copies, width):
    local = pl.BlockSpec(memory_space=pltpu.VMEM)
    return pl.pallas_call(
        second_product_kernel,
        in_specs=[local] * 3,
        out_specs=[local] * 2,
        out_shape=[
            jax.ShapeDtypeStruct(slope.shape, BF16),
            jax.ShapeDtypeStruct((copies, slope.shape[0], width), BF16),
        ],
        compiler_params=pltpu.CompilerParams(vmem_limit_bytes=1 << 20),
        name="second_product",
    )(backs, slope, rows)


def pack_kernel(*refs):
    *rows, out = refs
    out[...] = jnp.concatenate([r[...] for r in rows], 0)


def pack(rows):
    local = pl.BlockSpec(memory_space=pltpu.VMEM)
    shape = (len(rows) * rows[0].shape[0], rows[0].shape[1])
    return pl.pallas_call(
        pack_kernel,
        in_specs=[local] * len(rows),
        out_specs=local,
        out_shape=jax.ShapeDtypeStruct(shape, BF16),
        compiler_params=pltpu.CompilerParams(vmem_limit_bytes=2 << 20),
        name="pack",
    )(*rows)


def build_kernel(parts, second, *refs):
    *gees, out = refs
    nz, rows, wide = out.shape
    first = second[...].astype(F32) + parts[...].astype(F32).sum(0)
    late = jnp.concatenate([second[...].astype(F32), first], 0)
    piece = late.shape[1]
    n = gees[0].shape[1] // nz
    pairs = []
    for q in range((wide - piece) // n):
        pair = gees[2 * q : 2 * q + 2]
        pairs.append(jnp.concatenate([g[...].astype(F32) for g in (pair + pair)[:2]], 0))
    for z in range(nz):
        own = [p[:, z * n : (z + 1) * n] for p in pairs]
        out[z] = jnp.concatenate([late] + own, 1).astype(BF16)


def build(parts, second, gees, planes):
    local = pl.BlockSpec(memory_space=pltpu.VMEM)
    each, piece = second.shape
    wide = piece + (len(gees) + 1) // 2 * gees[0].shape[1] // planes
    return pl.pallas_call(
        build_kernel,
        in_specs=[local] * (2 + len(gees)),
        out_specs=local,
        out_shape=jax.ShapeDtypeStruct((planes, 2 * each, wide), BF16),
        compiler_params=pltpu.CompilerParams(vmem_limit_bytes=4 << 20),
        name="build",
    )(parts, second, *gees)


def finish_kernel(
    place, rows_early, rows_late, gee_last, base, left, right, inputs, early,
    in_grads, grad_in, grad_out,
    x_buf, e_buf, gees, pick_early, pick_late, sems,
):
    tok_rows, block = in_grads.shape
    per = gee_last.shape[1]
    step, steps = pl.program_id(0), pl.num_programs(0)
    nc, half, rows, piece = left.shape

    def both_cores(value):
        return value.reshape(nc * rows, piece)

    n = inputs.shape[1] * nc // tok_rows
    each = tok_rows // inputs.shape[0]
    bits = each.bit_length() - 1

    def pick(shape, width, first, fits=None):
        token = lax.broadcasted_iota(jnp.int32, shape, 0)
        col = lax.broadcasted_iota(jnp.int32, shape, 1)
        hit = col == (token >> bits) * width + first + (token & (each - 1))
        hit = hit if fits is None else hit & fits
        return jnp.where(hit, 1.0, 0.0).astype(BF16)

    part = block // inputs.shape[2]

    def copies(i):
        cols = pl.ds(pl.multiple_of(i * block, block), block)
        planes = inputs.shape[0] // nc
        yield pltpu.make_async_copy(early.at[:, cols], e_buf.at[i], sems.at[nc, i])
        for c in range(nc):
            yield pltpu.make_async_copy(
                inputs.at[pl.ds(c * planes + i * part, part)], x_buf.at[i, c], sems.at[c, i]
            )

    @pl.when(step == 0)
    def _():
        for i in range(x_buf.shape[0]):
            for copy in copies(i):
                copy.start()
        spot, core = place[0:1, 0:1], place[1:2, 0:1]
        pick_early[:tok_rows] = pick(
            (tok_rows, rows_early.shape[1]), (n - 2) * each, (n - 1 - spot) * each, spot > 1
        )
        pick_early[tok_rows:] = rows_early[...]
        pick_late[:tok_rows] = pick(
            (tok_rows, rows_late.shape[1]), 2 * each, (1 - spot) * each, spot < 2
        )
        pick_late[tok_rows:] = rows_late[...]
        shape = (piece, piece // nc)
        src = lax.broadcasted_iota(jnp.int32, shape, 0)
        dst = lax.broadcasted_iota(jnp.int32, shape, 1)
        low = per.bit_length() - 1
        own_core = src == ((dst >> low) * nc + core) * per + (dst & (per - 1))
        pick_core = jnp.where(own_core, 1.0, 0.0).astype(BF16)
        mine = dot(both_cores(right[:, half]), pick_core, ((1,), (0,))).astype(BF16)
        own = {n - 1: gee_last[...]}
        for j in range(2):
            found = dot(pick((tok_rows, nc * rows), 2 * each, j * each), mine, ((1,), (0,))).astype(BF16)
            for s in range(n - 2 - j, -1, -2):
                q = (n - 2 - j - s) // 2
                own[s] = found[:, q * per : (q + 1) * per]
        few = tok_rows // nc
        for c in range(nc):
            gees[c] = jnp.concatenate([own[s][c * few : (c + 1) * few] for s in range(n)], 0)

    for copy in copies(step):
        copy.wait()
    at = block // piece * (step % (steps // 2))
    late = jnp.concatenate(
        [
            jnp.where(step < steps // 2, both_cores(left[:, at + i]), both_cores(right[:, at + i]))
            for i in range(block // piece)
        ],
        1,
    )
    total = jnp.zeros(grad_in.shape, F32)
    for c in range(nc):
        x = jnp.concatenate([x_buf[step, c, k] for k in range(part)], 1)
        total += dot(gees[c], x, ((0,), (0,)))
    grad_in[...] = total
    found = dot(pick_early[...], e_buf[step], ((1,), (0,)))
    row = lax.broadcasted_iota(jnp.int32, late.shape, 0)
    second = jnp.where(row % 8 < 4, late.astype(F32), 0.0).astype(BF16)
    picked = dot(pick_late[:tok_rows], late, ((1,), (0,)))
    in_grads[...] = (found[:tok_rows] + picked).astype(BF16)
    grad_out[...] = (
        base[...] + found[tok_rows:] + dot(pick_late[tok_rows:], second, ((1,), (0,)))
    )


def finish(place, rows_early, rows_late, gee_last, base, left, right, inputs, early):
    per, width = base.shape
    tok_rows, nc = gee_last.shape[0], left.shape[0]
    steps = 4
    block = width // steps
    inputs = pltpu.with_memory_space_constraint(inputs, pltpu.HBM)
    early = pltpu.with_memory_space_constraint(early, pltpu.HBM)
    whole = lambda a: pl.BlockSpec(a.shape, lambda i: (0,) * a.ndim)
    cut = lambda rows: pl.BlockSpec((rows, block), lambda i: (0, i))
    return pl.pallas_call(
        finish_kernel,
        grid=(steps,),
        in_specs=[
            whole(place),
            whole(rows_early),
            whole(rows_late),
            whole(gee_last),
            cut(per),
            whole(left),
            whole(right),
            pl.BlockSpec(memory_space=pltpu.MemorySpace.HBM),
            pl.BlockSpec(memory_space=pltpu.MemorySpace.HBM),
        ],
        out_specs=[cut(tok_rows), cut(per), cut(per)],
        out_shape=[
            jax.ShapeDtypeStruct((tok_rows, width), BF16),
            jax.ShapeDtypeStruct((per, width), F32),
            jax.ShapeDtypeStruct((per, width), F32),
        ],
        scratch_shapes=[
            pltpu.VMEM((steps, nc, block // inputs.shape[2], *inputs.shape[1:]), BF16),
            pltpu.VMEM((steps, early.shape[0], block), BF16),
            pltpu.VMEM((nc, inputs.shape[1], per), BF16),
            pltpu.VMEM((tok_rows + per, rows_early.shape[1]), BF16),
            pltpu.VMEM((tok_rows + per, rows_late.shape[1]), BF16),
            pltpu.SemaphoreType.DMA((nc + 1, steps)),
        ],
        compiler_params=pltpu.CompilerParams(vmem_limit_bytes=24 << 20),
        name="finish",
    )(place, rows_early, rows_late, gee_last, base, left, right, inputs, early)


def body(layer_inputs, pre_act, out_grad, w_in, w_out):
    nc, nz = lax.axis_size("core"), lax.axis_size("z")
    sections, groups = size(SEC), nz * nc
    tok_rows, width = out_grad.shape
    per = w_in.shape[2]
    each = tok_rows // groups
    units = groups * per
    last = sections - 1
    own_in = w_in.reshape(per, width)
    own_out = w_out.reshape(per, width)
    spot = lax.axis_index(SEC)
    mine = lax.axis_index(TOK)

    both = lax.all_gather(jnp.concatenate([own_out, own_in], 0), HID, axis=0)

    own_pre = exchange(
        pre_act[0].reshape(tok_rows, sections, per).transpose(1, 0, 2), SEC
    )
    part = dot(out_grad, own_out, ((1,), (1,))).astype(BF16)
    back = lax.all_gather(part, "mp").astype(F32).sum(0)
    gee_last = (back * gelu_slope(own_pre[last].astype(F32))).astype(BF16)
    cuts = size(PLANE)
    branch = dot(gee_last, own_in, ((1,), (0,))).astype(BF16)
    branch = exchange(branch.reshape(tok_rows, cuts, -1).transpose(1, 0, 2), PLANE)
    branch = branch.astype(F32).sum(0).astype(BF16).reshape(groups, 1, each, LANES)
    some = sections // lax.axis_size("mp")
    sent = lax.dynamic_slice_in_dim(own_pre, lax.axis_index("mp") * some, some, 0)
    sent = sent.reshape(some, groups, each * per // LANES, LANES).transpose(1, 2, 0, 3)
    sent = jnp.concatenate([branch, sent], 1)
    hidden = jax.nn.gelu(own_pre.astype(F32), approximate=False).astype(BF16)
    hidden_rows = hidden[1:last].reshape(last - 1, groups, each, per)[::-1]
    hidden_rows = hidden_rows.transpose(3, 1, 0, 2).reshape(per, -1)
    hidden_late = hidden[0].T.reshape(per, groups, 1, each)
    hidden_late = jnp.pad(hidden_late, ((0, 0), (0, 0), (0, 1), (0, 0))).reshape(per, -1)
    place = jnp.stack([jnp.full((LANES,), spot), jnp.full((LANES,), lax.axis_index("core"))])
    base = dot(hidden[last], out_grad, ((0,), (0,)))

    ready = (place, pack([hidden_rows]), pack([hidden_late]), gee_last, base)
    got = exchange(sent, TOK)
    got, *ready = fence(got, *ready)
    branch = got[:, 0].reshape(nc, nz, each, LANES).astype(F32).sum(1).astype(BF16)
    branch = shared(branch.transpose(1, 0, 2).reshape(each, nc * LANES), ROWS)
    total = branch.transpose(1, 0, 2).reshape(each, width)
    pre = lax.all_gather(got[:, 1], "mp", axis=0)
    pre = pre.reshape(-1, nc, nz, some, each, per).transpose(0, 3, 4, 2, 1, 5)
    pre = pre.reshape(sections, each, units)[:last]
    inputs, total, pre = fence(layer_inputs[0], total, pre)
    inputs = lax.dynamic_slice_in_dim(
        inputs, lax.axis_index("z") * (width // nz), width // nz, 1, allow_negative_indices=False
    )
    inputs = jnp.broadcast_to(
        inputs.reshape(1, nc, tok_rows // nc, width // nz),
        (sections // nc, nc, tok_rows // nc, width // nz),
    )
    inputs = exchange(inputs.reshape(sections, tok_rows // nc, width // nz), SEC)
    slopes = gelu_slope(pre.reshape(last, each, units).astype(F32))
    upper = lax.dynamic_slice_in_dim(out_grad, mine * each, each, 0)
    upper = (upper.astype(F32) + total.astype(F32)).astype(BF16)
    slopes = [slopes[s] for s in range(last)]
    cuts = size(ROWS)
    piece = width // cuts
    cut = lax.axis_index(ROWS) * piece
    inputs = lax.all_gather(inputs.reshape(-1, width // nz), TOK, axis=0)
    both, upper, cut, *ready = fence(both, upper, cut, *ready, *slopes)
    ready, slopes = ready[:-last], ready[-last:]
    *cols_out, rows_in, part = fence(*unpack(both, upper))

    gees, results = [], [upper]
    for s in reversed(range(last)):
        backs = lax.all_gather(part, "mp")
        gee, sent = fence(
            *second_product(backs, slopes[s], rows_in, cuts, width if s > 0 else piece)
        )
        gees.append(gee)
        if s == 2:
            parts = exchange(sent, ROWS)
            upper = (upper.astype(F32) + parts.astype(F32).sum(0)).astype(BF16)
            results.append(fence(upper))
            early = lax.all_gather(pack(results), TOK, axis=0)
            early = early.reshape(groups * (last - 1) * each, width)
            upper, part, kept = fence(*reading_product(parts, results[-2], *cols_out))
            cols_out = [cols_out[0], kept]
        elif s > 0:
            upper, part = fence(*product(exchange(sent, ROWS), upper, cols_out))
            results.append(upper)

    second = lax.dynamic_slice_in_dim(
        upper, cut, piece, 1, allow_negative_indices=False
    )
    sent, second = fence(sent, second)
    total = exchange(sent, ROWS)
    late = build(total, second, gees, nz)
    late = exchange(late, "z")
    gs = late[:, :, piece:]
    late = shared(late[:, :, :piece], ROWS)
    left = lax.all_gather(late[: cuts // 2], "core", axis=0)
    right = lax.all_gather(jnp.concatenate([late[cuts // 2 :], gs[None]], 0), "core", axis=0)
    in_grads, grad_in, grad_out = finish(
        *ready,
        left.reshape(nc, cuts // 2, -1, piece),
        right.reshape(nc, cuts // 2 + 1, -1, piece),
        inputs,
        early,
    )
    return (
        in_grads.reshape(1, tok_rows, width),
        grad_in.reshape(w_in.shape),
        grad_out.reshape(w_out.shape),
    )


def solution(mesh):
    split = Mesh(
        mesh.devices.reshape(
            mesh.shape["section"] // 2, 2, mesh.shape["dp"] // 2, 2, mesh.shape["mp"]
        ),
        ("x", "core", "z", "yl", "mp"),
    )
    placed = (
        P(SEC, None, "mp"),
        P(SEC, None, DP),
        P(None, "mp"),
        P(DP, SEC, None, "mp"),
        P(DP, SEC, None, "mp"),
    )
    return jax.shard_map(
        body,
        mesh=split,
        in_specs=placed,
        out_specs=(P(SEC, None, "mp"), P(DP, SEC, None, "mp"), P(DP, SEC, None, "mp")),
        check_vma=False,
    )
```

```python
import jax
import jax.numpy as jnp
from jax import lax
from jax.experimental import pallas as pl
from jax.experimental.pallas import tpu as pltpu
from jax.sharding import Mesh
from jax.sharding import PartitionSpec as P

F32 = jnp.float32
BF16 = jnp.bfloat16
LANES = 128
PARTS = (2, 2)
SEC = ("x", "core")
DP = ("z", "yl")
TOK = ("core", "z")
HID = ("z", "core")
ROWS = ("x", "yl")
PLANE = ("x", "yl", "core")


def size(axes):
    n = 1
    for a in axes:
        n *= lax.axis_size(a)
    return n


def exchange(value, axes):
    return lax.all_to_all(value, axes, 0, 0, tiled=True)


def shared(value, axes):
    n = size(axes)
    return exchange(jnp.broadcast_to(value[None], (n,) + value.shape), axes)


def fence(*values):
    return lax.optimization_barrier(values if len(values) > 1 else values[0])


def gelu_slope(value):
    cdf = 0.5 * (1.0 + lax.erf(value * 0.7071067811865476))
    dens = jnp.exp(-0.5 * value * value) * 0.3989422804014327
    return cdf + value * dens


def dot(left, right, dims):
    return lax.dot_general(left, right, (dims, ((), ())), preferred_element_type=F32)


def unpack_kernel(both, upper, *refs):
    *cols_out, rows_in, part, buf, sems = refs
    groups, two, width = both.shape
    per = two // 2
    cut = sems.shape[1]
    n = groups // cut
    homes = [
        c.at[:, pl.ds(i * n * per, n * per)]
        for c in cols_out
        for i in range(c.shape[1] // (n * per))
    ]

    def copy(w, i, ref):
        return pltpu.make_async_copy(
            both.at[pl.ds(i * n, n), pl.ds(w * per, per)],
            ref.at[pl.ds(i * n, n)],
            sems.at[w, i],
        )

    copies = [copy(0, i, buf) for i in range(cut)]
    others = [copy(1, i, rows_in) for i in range(cut)]
    for c in copies + others:
        c.start()
    for i, c in enumerate(copies):
        c.wait()
        at = slice(i * n * per, (i + 1) * n * per)
        cols = buf[i * n : (i + 1) * n].reshape(n * per, width).T
        homes[i][...] = cols
        part[:, at] = dot(upper[...], cols, ((1,), (0,))).astype(BF16)
    for c in others:
        c.wait()


def unpack(both, upper):
    groups, two, width = both.shape
    units = groups * two // 2
    local = pl.BlockSpec(memory_space=pltpu.VMEM)
    rows = (groups, two // 2, width)
    cut = 4
    *cols_out, rows_in, part = pl.pallas_call(
        unpack_kernel,
        in_specs=[pl.BlockSpec(memory_space=pltpu.MemorySpace.HBM), local],
        out_specs=[local] * (len(PARTS) + 2),
        out_shape=[jax.ShapeDtypeStruct((width, units // cut * k), BF16) for k in PARTS]
        + [
            jax.ShapeDtypeStruct(rows, BF16),
            jax.ShapeDtypeStruct((upper.shape[0], units), BF16),
        ],
        scratch_shapes=[pltpu.VMEM(rows, BF16), pltpu.SemaphoreType.DMA((2, cut))],
        compiler_params=pltpu.CompilerParams(vmem_limit_bytes=8 << 20),
        name="unpack",
    )(pltpu.with_memory_space_constraint(both, pltpu.HBM), upper)
    return (*cols_out, rows_in.reshape(units, width), part)


def product_kernel(parts, upper, *refs):
    *cols, total, part = refs
    total[...] = (upper[...].astype(F32) + parts[...].astype(F32).sum(0)).astype(BF16)
    at = 0
    for c in cols:
        n = c.shape[1]
        part[:, at : at + n] = dot(total[...], c[...], ((1,), (0,))).astype(BF16)
        at += n


def product(parts, upper, cols):
    local = pl.BlockSpec(memory_space=pltpu.VMEM)
    units = sum(c.shape[1] for c in cols)
    return pl.pallas_call(
        product_kernel,
        in_specs=[local] * (2 + len(cols)),
        out_specs=[local] * 2,
        out_shape=[
            jax.ShapeDtypeStruct(upper.shape, BF16),
            jax.ShapeDtypeStruct((upper.shape[0], units), BF16),
        ],
        compiler_params=pltpu.CompilerParams(vmem_limit_bytes=1 << 20),
        name="product",
    )(parts, upper, *cols)


def reading_product_kernel(parts, upper, near, far, total, part, buf, sems):
    cut = sems.shape[0]
    n = far.shape[0] // cut
    copies = [
        pltpu.make_async_copy(far.at[pl.ds(i * n, n)], buf.at[pl.ds(i * n, n)], sems.at[i])
        for i in range(cut)
    ]
    for copy in copies:
        copy.start()
    total[...] = (upper[...].astype(F32) + parts[...].astype(F32).sum(0)).astype(BF16)
    units = near.shape[1]
    part[:, :units] = dot(total[...], near[...], ((1,), (0,))).astype(BF16)
    value = jnp.zeros((upper.shape[0], far.shape[1]), F32)
    for i, copy in enumerate(copies):
        copy.wait()
        at = slice(i * n, (i + 1) * n)
        value += dot(total[:, at], buf[at], ((1,), (0,)))
    part[:, units:] = value.astype(BF16)


def reading_product(parts, upper, near, far):
    local = pl.BlockSpec(memory_space=pltpu.VMEM)
    units = near.shape[1] + far.shape[1]
    return pl.pallas_call(
        reading_product_kernel,
        in_specs=[local] * 3 + [pl.BlockSpec(memory_space=pltpu.MemorySpace.HBM)],
        out_specs=[local] * 3,
        out_shape=[
            jax.ShapeDtypeStruct(upper.shape, BF16),
            jax.ShapeDtypeStruct((upper.shape[0], units), BF16),
            jax.ShapeDtypeStruct(far.shape, BF16),
        ],
        scratch_shapes=[pltpu.SemaphoreType.DMA((4,))],
        compiler_params=pltpu.CompilerParams(vmem_limit_bytes=4 << 20),
        name="reading_product",
    )(parts, upper, near, pltpu.with_memory_space_constraint(far, pltpu.HBM))


def second_product_kernel(backs, slope, rows, gee, sent):
    value = (backs[0].astype(F32) + backs[1].astype(F32)) * slope[...]
    gee[...] = value.astype(BF16)
    branch = dot(gee[...], rows[...], ((1,), (0,))).astype(BF16)
    n = sent.shape[2]
    for i in range(sent.shape[0]):
        at = i * n % branch.shape[1]
        sent[i] = branch[:, at : at + n]


def second_product(backs, slope, rows, copies, width):
    local = pl.BlockSpec(memory_space=pltpu.VMEM)
    return pl.pallas_call(
        second_product_kernel,
        in_specs=[local] * 3,
        out_specs=[local] * 2,
        out_shape=[
            jax.ShapeDtypeStruct(slope.shape, BF16),
            jax.ShapeDtypeStruct((copies, slope.shape[0], width), BF16),
        ],
        compiler_params=pltpu.CompilerParams(vmem_limit_bytes=1 << 20),
        name="second_product",
    )(backs, slope, rows)


def pack_kernel(*refs):
    *rows, out = refs
    out[...] = jnp.concatenate([r[...] for r in rows], 0)


def pack(rows):
    local = pl.BlockSpec(memory_space=pltpu.VMEM)
    shape = (len(rows) * rows[0].shape[0], rows[0].shape[1])
    return pl.pallas_call(
        pack_kernel,
        in_specs=[local] * len(rows),
        out_specs=local,
        out_shape=jax.ShapeDtypeStruct(shape, BF16),
        compiler_params=pltpu.CompilerParams(vmem_limit_bytes=2 << 20),
        name="pack",
    )(*rows)


def build_kernel(parts, second, *refs):
    *gees, out = refs
    nz, rows, wide = out.shape
    first = second[...].astype(F32) + parts[...].astype(F32).sum(0)
    late = jnp.concatenate([second[...].astype(F32), first], 0)
    piece = late.shape[1]
    n = gees[0].shape[1] // nz
    pairs = []
    for q in range((wide - piece) // n):
        pair = gees[2 * q : 2 * q + 2]
        pairs.append(jnp.concatenate([g[...].astype(F32) for g in (pair + pair)[:2]], 0))
    for z in range(nz):
        own = [p[:, z * n : (z + 1) * n] for p in pairs]
        out[z] = jnp.concatenate([late] + own, 1).astype(BF16)


def build(parts, second, gees, planes):
    local = pl.BlockSpec(memory_space=pltpu.VMEM)
    each, piece = second.shape
    wide = piece + (len(gees) + 1) // 2 * gees[0].shape[1] // planes
    return pl.pallas_call(
        build_kernel,
        in_specs=[local] * (2 + len(gees)),
        out_specs=local,
        out_shape=jax.ShapeDtypeStruct((planes, 2 * each, wide), BF16),
        compiler_params=pltpu.CompilerParams(vmem_limit_bytes=4 << 20),
        name="build",
    )(parts, second, *gees)


def finish_kernel(
    place, rows_early, rows_late, gee_last, base, left, right, inputs, early,
    in_grads, grad_in, grad_out,
    x_buf, e_buf, gees, pick_early, pick_late, sems,
):
    tok_rows, block = in_grads.shape
    per = gee_last.shape[1]
    step, steps = pl.program_id(0), pl.num_programs(0)
    nc, half, rows, piece = left.shape

    def both_cores(value):
        return value.reshape(nc * rows, piece)

    n = inputs.shape[1] * nc // tok_rows
    each = tok_rows // inputs.shape[0]
    bits = each.bit_length() - 1

    def pick(shape, width, first, fits=None):
        token = lax.broadcasted_iota(jnp.int32, shape, 0)
        col = lax.broadcasted_iota(jnp.int32, shape, 1)
        hit = col == (token >> bits) * width + first + (token & (each - 1))
        hit = hit if fits is None else hit & fits
        return jnp.where(hit, 1.0, 0.0).astype(BF16)

    part = block // inputs.shape[2]

    def copies(i):
        cols = pl.ds(pl.multiple_of(i * block, block), block)
        planes = inputs.shape[0] // nc
        yield pltpu.make_async_copy(early.at[:, cols], e_buf.at[i], sems.at[nc, i])
        for c in range(nc):
            yield pltpu.make_async_copy(
                inputs.at[pl.ds(c * planes + i * part, part)], x_buf.at[i, c], sems.at[c, i]
            )

    @pl.when(step == 0)
    def _():
        for i in range(x_buf.shape[0]):
            for copy in copies(i):
                copy.start()
        spot, core = place[0:1, 0:1], place[1:2, 0:1]
        pick_early[:tok_rows] = pick(
            (tok_rows, rows_early.shape[1]), (n - 2) * each, (n - 1 - spot) * each, spot > 1
        )
        pick_early[tok_rows:] = rows_early[...]
        pick_late[:tok_rows] = pick(
            (tok_rows, rows_late.shape[1]), 2 * each, (1 - spot) * each, spot < 2
        )
        pick_late[tok_rows:] = rows_late[...]
        shape = (piece, piece // nc)
        src = lax.broadcasted_iota(jnp.int32, shape, 0)
        dst = lax.broadcasted_iota(jnp.int32, shape, 1)
        low = per.bit_length() - 1
        own_core = src == ((dst >> low) * nc + core) * per + (dst & (per - 1))
        pick_core = jnp.where(own_core, 1.0, 0.0).astype(BF16)
        mine = dot(both_cores(right[:, half]), pick_core, ((1,), (0,))).astype(BF16)
        own = {n - 1: gee_last[...]}
        for j in range(2):
            found = dot(pick((tok_rows, nc * rows), 2 * each, j * each), mine, ((1,), (0,))).astype(BF16)
            for s in range(n - 2 - j, -1, -2):
                q = (n - 2 - j - s) // 2
                own[s] = found[:, q * per : (q + 1) * per]
        few = tok_rows // nc
        for c in range(nc):
            gees[c] = jnp.concatenate([own[s][c * few : (c + 1) * few] for s in range(n)], 0)

    for copy in copies(step):
        copy.wait()
    at = block // piece * (step % (steps // 2))
    late = jnp.concatenate(
        [
            jnp.where(step < steps // 2, both_cores(left[:, at + i]), both_cores(right[:, at + i]))
            for i in range(block // piece)
        ],
        1,
    )
    total = jnp.zeros(grad_in.shape, F32)
    for c in range(nc):
        x = jnp.concatenate([x_buf[step, c, k] for k in range(part)], 1)
        total += dot(gees[c], x, ((0,), (0,)))
    grad_in[...] = total
    found = dot(pick_early[...], e_buf[step], ((1,), (0,)))
    row = lax.broadcasted_iota(jnp.int32, late.shape, 0)
    second = jnp.where(row % 8 < 4, late.astype(F32), 0.0).astype(BF16)
    picked = dot(pick_late[:tok_rows], late, ((1,), (0,)))
    in_grads[...] = (found[:tok_rows] + picked).astype(BF16)
    grad_out[...] = (
        base[...] + found[tok_rows:] + dot(pick_late[tok_rows:], second, ((1,), (0,)))
    )


def finish(place, rows_early, rows_late, gee_last, base, left, right, inputs, early):
    per, width = base.shape
    tok_rows, nc = gee_last.shape[0], left.shape[0]
    steps = 4
    block = width // steps
    inputs = pltpu.with_memory_space_constraint(inputs, pltpu.HBM)
    early = pltpu.with_memory_space_constraint(early, pltpu.HBM)
    local = pl.BlockSpec(memory_space=pltpu.VMEM)
    cut = lambda rows: pl.BlockSpec((rows, block), lambda i: (0, i))
    return pl.pallas_call(
        finish_kernel,
        grid=(steps,),
        in_specs=[
            local,
            local,
            local,
            local,
            cut(per),
            local,
            local,
            pl.BlockSpec(memory_space=pltpu.MemorySpace.HBM),
            pl.BlockSpec(memory_space=pltpu.MemorySpace.HBM),
        ],
        out_specs=[cut(tok_rows), cut(per), cut(per)],
        out_shape=[
            jax.ShapeDtypeStruct((tok_rows, width), BF16),
            jax.ShapeDtypeStruct((per, width), F32),
            jax.ShapeDtypeStruct((per, width), F32),
        ],
        scratch_shapes=[
            pltpu.VMEM((steps, nc, block // inputs.shape[2], *inputs.shape[1:]), BF16),
            pltpu.VMEM((steps, early.shape[0], block), BF16),
            pltpu.VMEM((nc, inputs.shape[1], per), BF16),
            pltpu.VMEM((tok_rows + per, rows_early.shape[1]), BF16),
            pltpu.VMEM((tok_rows + per, rows_late.shape[1]), BF16),
            pltpu.SemaphoreType.DMA((nc + 1, steps)),
        ],
        compiler_params=pltpu.CompilerParams(vmem_limit_bytes=24 << 20),
        name="finish",
    )(place, rows_early, rows_late, gee_last, base, left, right, inputs, early)


def body(layer_inputs, pre_act, out_grad, w_in, w_out):
    nc, nz = lax.axis_size("core"), lax.axis_size("z")
    sections, groups = size(SEC), nz * nc
    tok_rows, width = out_grad.shape
    per = w_in.shape[2]
    each = tok_rows // groups
    units = groups * per
    last = sections - 1
    own_in = w_in.reshape(per, width)
    own_out = w_out.reshape(per, width)
    spot = lax.axis_index(SEC)
    mine = lax.axis_index(TOK)

    both = lax.all_gather(jnp.concatenate([own_out, own_in], 0), HID, axis=0)

    own_pre = exchange(
        pre_act[0].reshape(tok_rows, sections, per).transpose(1, 0, 2), SEC
    )
    part = dot(out_grad, own_out, ((1,), (1,))).astype(BF16)
    back = lax.all_gather(part, "mp").astype(F32).sum(0)
    gee_last = (back * gelu_slope(own_pre[last].astype(F32))).astype(BF16)
    cuts = size(PLANE)
    branch = dot(gee_last, own_in, ((1,), (0,))).astype(BF16)
    branch = exchange(branch.reshape(tok_rows, cuts, -1).transpose(1, 0, 2), PLANE)
    branch = branch.astype(F32).sum(0).astype(BF16).reshape(groups, 1, each, LANES)
    some = sections // lax.axis_size("mp")
    sent = lax.dynamic_slice_in_dim(own_pre, lax.axis_index("mp") * some, some, 0)
    sent = sent.reshape(some, groups, each * per // LANES, LANES).transpose(1, 2, 0, 3)
    sent = jnp.concatenate([branch, sent], 1)
    hidden = jax.nn.gelu(own_pre.astype(F32), approximate=False).astype(BF16)
    hidden_rows = hidden[1:last].reshape(last - 1, groups, each, per)[::-1]
    hidden_rows = hidden_rows.transpose(3, 1, 0, 2).reshape(per, -1)
    hidden_late = hidden[0].T.reshape(per, groups, 1, each)
    hidden_late = jnp.pad(hidden_late, ((0, 0), (0, 0), (0, 1), (0, 0))).reshape(per, -1)
    place = jnp.stack([jnp.full((LANES,), spot), jnp.full((LANES,), lax.axis_index("core"))])
    base = dot(hidden[last], out_grad, ((0,), (0,)))

    ready = (place, pack([hidden_rows]), pack([hidden_late]), gee_last, base)
    got = exchange(sent, TOK)
    got, *ready = fence(got, *ready)
    branch = got[:, 0].reshape(nc, nz, each, LANES).astype(F32).sum(1).astype(BF16)
    branch = shared(branch.transpose(1, 0, 2).reshape(each, nc * LANES), ROWS)
    total = branch.transpose(1, 0, 2).reshape(each, width)
    pre = lax.all_gather(got[:, 1], "mp", axis=0)
    pre = pre.reshape(-1, nc, nz, some, each, per).transpose(0, 3, 4, 2, 1, 5)
    pre = pre.reshape(sections, each, units)[:last]
    inputs, total, pre = fence(layer_inputs[0], total, pre)
    inputs = lax.dynamic_slice_in_dim(
        inputs, lax.axis_index("z") * (width // nz), width // nz, 1, allow_negative_indices=False
    )
    inputs = jnp.broadcast_to(
        inputs.reshape(1, nc, tok_rows // nc, width // nz),
        (sections // nc, nc, tok_rows // nc, width // nz),
    )
    inputs = exchange(inputs.reshape(sections, tok_rows // nc, width // nz), SEC)
    slopes = gelu_slope(pre.reshape(last, each, units).astype(F32))
    upper = lax.dynamic_slice_in_dim(out_grad, mine * each, each, 0)
    upper = (upper.astype(F32) + total.astype(F32)).astype(BF16)
    slopes = [slopes[s] for s in range(last)]
    cuts = size(ROWS)
    piece = width // cuts
    cut = lax.axis_index(ROWS) * piece
    inputs = lax.all_gather(inputs.reshape(-1, width // nz), TOK, axis=0)
    both, upper, cut, *ready = fence(both, upper, cut, *ready, *slopes)
    ready, slopes = ready[:-last], ready[-last:]
    *cols_out, rows_in, part = fence(*unpack(both, upper))

    gees, results = [], [upper]
    for s in reversed(range(last)):
        backs = lax.all_gather(part, "mp")
        gee, sent = fence(
            *second_product(backs, slopes[s], rows_in, cuts, width if s > 0 else piece)
        )
        gees.append(gee)
        if s == 2:
            parts = exchange(sent, ROWS)
            upper = (upper.astype(F32) + parts.astype(F32).sum(0)).astype(BF16)
            results.append(fence(upper))
            early = lax.all_gather(pack(results), TOK, axis=0)
            early = early.reshape(groups * (last - 1) * each, width)
            upper, part, kept = fence(*reading_product(parts, results[-2], *cols_out))
            cols_out = [cols_out[0], kept]
        elif s > 0:
            upper, part = fence(*product(exchange(sent, ROWS), upper, cols_out))
            results.append(upper)

    second = lax.dynamic_slice_in_dim(
        upper, cut, piece, 1, allow_negative_indices=False
    )
    sent, second = fence(sent, second)
    total = exchange(sent, ROWS)
    late = build(total, second, gees, nz)
    late = exchange(late, "z")
    gs = late[:, :, piece:]
    late = shared(late[:, :, :piece], ROWS)
    left = lax.all_gather(late[: cuts // 2], "core", axis=0)
    right = lax.all_gather(jnp.concatenate([late[cuts // 2 :], gs[None]], 0), "core", axis=0)
    in_grads, grad_in, grad_out = finish(
        *ready,
        left.reshape(nc, cuts // 2, -1, piece),
        right.reshape(nc, cuts // 2 + 1, -1, piece),
        inputs,
        early,
    )
    return (
        in_grads.reshape(1, tok_rows, width),
        grad_in.reshape(w_in.shape),
        grad_out.reshape(w_out.shape),
    )


def solution(mesh):
    split = Mesh(
        mesh.devices.reshape(
            mesh.shape["section"] // 2, 2, mesh.shape["dp"] // 2, 2, mesh.shape["mp"]
        ),
        ("x", "core", "z", "yl", "mp"),
    )
    placed = (
        P(SEC, None, "mp"),
        P(SEC, None, DP),
        P(None, "mp"),
        P(DP, SEC, None, "mp"),
        P(DP, SEC, None, "mp"),
    )
    return jax.shard_map(
        body,
        mesh=split,
        in_specs=placed,
        out_specs=(P(SEC, None, "mp"), P(DP, SEC, None, "mp"), P(DP, SEC, None, "mp")),
        check_vma=False,
    )
```
